16 devices in a mesh: tp: 2 (over z), dp: 8 (over y, x, core).
Axes of the slice: x: 2, y: 2, z: 2, core: 2. Of those that a mesh axis runs over, the one named last changes fastest.
Arguments:
- feats: bfloat16 [4096, 49, 1024], P('dp')
- ln_gamma: float32 [1024], replicated
- ln_beta: float32 [1024], replicated
- w_head: bfloat16 [1024, 22528], P(None, 'tp')
- b_head: float32 [22528], P('tp')
- labels: int32 [4096], P('dp')
Outputs:
- output 1: float32 [], replicated
- output 2: bfloat16 [4096, 49, 1024], P('dp')
- output 3: float32 [1024, 22528], P(None, 'tp')
- output 4: float32 [22528], P('tp')
- output 5: float32 [1024], replicated
- output 6: float32 [1024], replicated
All inputs are finite; a program needn't handle non-finite values.
Results may differ from the reference program's by a relative error of at most 0.001.
Values sent between devices are 32-bit elements.
A program may use at most 1 GiB of HBM per device.

```python
import jax
import jax.numpy as jnp
from jax import lax

GLOBAL_BATCH = 4096
TOKENS = 49
WIDTH = 1024
CLASSES = 21841
PADDED_CLASSES = 22528
ROW_BLOCK = min(GLOBAL_BATCH, 64)
LN_EPS = 1e-5
SMOOTH = 0.1


def setup_inputs(seed: int = 0) -> dict:
    sub_keys = jax.random.split(jax.random.key(seed), 7)
    image_shared = jax.random.normal(sub_keys[0], (GLOBAL_BATCH, 1, WIDTH), jnp.float32)
    token_noise = jax.random.normal(sub_keys[1], (GLOBAL_BATCH, TOKENS, WIDTH), jnp.float32)
    feats = (image_shared + 0.5 * token_noise).astype(jnp.bfloat16)
    ln_gamma = 1.0 + 0.3 * jax.random.normal(sub_keys[2], (WIDTH,), jnp.float32)
    ln_beta = 0.3 * jax.random.normal(sub_keys[3], (WIDTH,), jnp.float32)
    w_scale = 3.0 * WIDTH ** -0.5
    w_head = (w_scale * jax.random.normal(sub_keys[4], (WIDTH, PADDED_CLASSES), jnp.float32)).astype(jnp.bfloat16)
    b_head = 0.5 * jax.random.normal(sub_keys[5], (PADDED_CLASSES,), jnp.float32)
    labels = jax.random.randint(sub_keys[6], (GLOBAL_BATCH,), 0, CLASSES, dtype=jnp.int32)
    labels = labels.at[0].set(0).at[GLOBAL_BATCH - 1].set(CLASSES - 1)
    return {"feats": feats, "ln_gamma": ln_gamma, "ln_beta": ln_beta, "w_head": w_head, "b_head": b_head, "labels": labels}


def norm_pool(feats, ln_gamma, ln_beta):
    x_val = feats.astype(jnp.float32)
    mean_x = jnp.mean(x_val, axis=-1, keepdims=True)
    centered = x_val - mean_x
    var_x = jnp.mean(centered * centered, axis=-1, keepdims=True)
    inv_std = lax.rsqrt(var_x + LN_EPS)
    x_hat = centered * inv_std
    x_hat_mean = jnp.mean(x_hat, axis=1)
    pooled16 = (x_hat_mean * ln_gamma + ln_beta).astype(jnp.bfloat16)
    return x_hat, inv_std, x_hat_mean, pooled16


def norm_backward(grad_pool, x_hat, inv_std, x_hat_mean, ln_gamma):
    grad_gamma = jnp.sum(grad_pool * x_hat_mean, axis=0)
    grad_beta = jnp.sum(grad_pool, axis=0)
    upstream = grad_pool * ln_gamma / TOKENS
    up_mean = jnp.mean(upstream, axis=-1)
    proj_term = jnp.mean(x_hat * upstream[:, None, :], axis=-1, keepdims=True)
    grad_x = inv_std * (upstream[:, None, :] - up_mean[:, None, None] - x_hat * proj_term)
    return grad_x.astype(jnp.bfloat16), grad_gamma, grad_beta


def head_rows(feat_rows, label_rows, ln_gamma, ln_beta, w_head, b_head):
    x_hat, inv_std, x_hat_mean, pooled16 = norm_pool(feat_rows, ln_gamma, ln_beta)
    col_ids = jnp.arange(PADDED_CLASSES)
    valid_mask = col_ids < CLASSES
    logits = jnp.dot(pooled16, w_head, preferred_element_type=jnp.float32) + b_head
    logits = jnp.where(valid_mask, logits, -1e30)
    row_max = jnp.max(logits, axis=-1, keepdims=True)
    log_norm = row_max + jnp.log(jnp.sum(jnp.exp(logits - row_max), axis=-1, keepdims=True))
    onehot = col_ids == label_rows[:, None]
    target = jnp.sum(jnp.where(onehot, logits, 0.0), axis=-1)
    valid_sum = jnp.sum(jnp.where(valid_mask, logits, 0.0), axis=-1)
    loss_rows = log_norm[:, 0] - (1.0 - SMOOTH) * target - (SMOOTH / CLASSES) * valid_sum
    soft_probs = jnp.exp(logits - log_norm)
    dlogit = (soft_probs - (1.0 - SMOOTH) * onehot - (SMOOTH / CLASSES) * valid_mask) / GLOBAL_BATCH
    dlogit16 = dlogit.astype(jnp.bfloat16)
    grad_w = jnp.dot(pooled16.T, dlogit16, preferred_element_type=jnp.float32)
    grad_b = jnp.sum(dlogit, axis=0)
    grad_pool = jnp.dot(dlogit16, w_head.T, preferred_element_type=jnp.float32)
    grad_x, grad_gamma, grad_beta = norm_backward(grad_pool, x_hat, inv_std, x_hat_mean, ln_gamma)
    return jnp.sum(loss_rows), grad_x, grad_w, grad_b, grad_gamma, grad_beta


def reference(feats, ln_gamma, ln_beta, w_head, b_head, labels):
    block_count = GLOBAL_BATCH // ROW_BLOCK
    feat_blocks = feats.reshape(block_count, ROW_BLOCK, TOKENS, WIDTH)
    label_blocks = labels.reshape(block_count, ROW_BLOCK)
    init_carry = (jnp.zeros((), jnp.float32), jnp.zeros((WIDTH, PADDED_CLASSES), jnp.float32), jnp.zeros((PADDED_CLASSES,), jnp.float32), jnp.zeros((WIDTH,), jnp.float32), jnp.zeros((WIDTH,), jnp.float32))

    def scan_step(acc_carry, block_in):
        loss_sum, grad_x, grad_w, grad_b, grad_gamma, grad_beta = head_rows(block_in[0], block_in[1], ln_gamma, ln_beta, w_head, b_head)
        new_carry = (acc_carry[0] + loss_sum, acc_carry[1] + grad_w, acc_carry[2] + grad_b, acc_carry[3] + grad_gamma, acc_carry[4] + grad_beta)
        return new_carry, grad_x

    final_carry, grad_blocks = lax.scan(scan_step, init_carry, (feat_blocks, label_blocks))
    grad_feats = grad_blocks.reshape(GLOBAL_BATCH, TOKENS, WIDTH)
    return (final_carry[0] / GLOBAL_BATCH, grad_feats, final_carry[1], final_carry[2], final_carry[3], final_carry[4])
```

```python
import functools

import jax
import jax.numpy as jnp
from jax import lax
from jax.experimental import pallas as pl
from jax.experimental.pallas import tpu as pltpu
from jax.sharding import PartitionSpec as P


VALID = 21841
LN_EPS = 1e-5
SMOOTH = 0.1
F32 = jnp.float32
BF16 = jnp.bfloat16
MIB = 2**20


def _cost(flops, nbytes):
    return pl.CostEstimate(flops=int(flops), bytes_accessed=int(nbytes), transcendentals=0)


def _ln_kernel(f_ref, g_ref, b_ref, p_ref, xm_ref, mean_ref, inv_ref, *, rows, sub, group):
    lane = lax.broadcasted_iota(jnp.int32, (sub, 128), 1)
    tokens, _, width = f_ref.shape
    ones = jnp.ones((width, 128), BF16)

    def step(s, carry):
        r = pl.ds(pl.multiple_of(s * sub, sub), sub)
        acc = jnp.zeros((sub, width), F32)
        means = jnp.zeros((sub, 128), F32)
        invs = jnp.zeros((sub, 128), F32)
        for t0 in range(0, tokens, group):
            xb = f_ref[t0 : t0 + group, r, :].reshape(group * sub, width)
            mu_all = jnp.dot(xb, ones, preferred_element_type=F32) * (1.0 / width)
            mus, ivs = [], []
            for j in range(group):
                mu = mu_all[j * sub : (j + 1) * sub, :]
                x = f_ref[t0 + j, r, :].astype(F32)
                q = jnp.zeros((sub, 128), F32)
                for k in range(width // 128):
                    d = x[:, k * 128 : (k + 1) * 128] - mu
                    q = q + d * d
                var = jnp.sum(q, -1, keepdims=True) * (1.0 / width)
                mus.append(mu)
                ivs.append(lax.rsqrt(var + LN_EPS))
            for j in range(group):
                x = f_ref[t0 + j, r, :].astype(F32)
                hats = [(x[:, k * 128 : (k + 1) * 128] - mus[j]) * ivs[j] for k in range(width // 128)]
                acc = acc + jnp.concatenate(hats, 1)
                hit = lane == t0 + j
                means = jnp.where(hit, mus[j], means)
                invs = jnp.where(hit, ivs[j], invs)
        xm = acc * (1.0 / tokens)
        xm_ref[r, :] = xm
        p_ref[r, :] = (xm * g_ref[...] + b_ref[...]).astype(BF16).astype(F32)
        mean_ref[r, :] = means
        inv_ref[r, :] = invs
        return carry

    lax.fori_loop(0, rows // sub, step, 0)


def _ln_forward(ft, gamma, beta, rows=32, sub=32, group=7):
    tokens, images, width = ft.shape
    return pl.pallas_call(
        functools.partial(_ln_kernel, rows=rows, sub=sub, group=group),
        grid=(images // rows,),
        in_specs=[
            pl.BlockSpec((tokens, rows, width), lambda i: (0, i, 0)),
            pl.BlockSpec((1, width), lambda i: (0, 0)),
            pl.BlockSpec((1, width), lambda i: (0, 0)),
        ],
        out_specs=[pl.BlockSpec((rows, width), lambda i: (i, 0))] * 2 + [pl.BlockSpec((rows, 128), lambda i: (i, 0))] * 2,
        out_shape=[jax.ShapeDtypeStruct((images, width), F32)] * 2 + [jax.ShapeDtypeStruct((images, 128), F32)] * 2,
        compiler_params=pltpu.CompilerParams(vmem_limit_bytes=60 * MIB),
        cost_estimate=_cost(36e-6 * 996e12, tokens * images * width * 2),
        name="ln_forward",
    )(ft, gamma, beta)


def _df_kernel(f_ref, da_ref, db_ref, g_ref, mean_ref, inv_ref, o_ref, *, rows, sub, group):
    tokens, _, width = f_ref.shape

    def step(s, carry):
        r = pl.ds(pl.multiple_of(s * sub, sub), sub)
        up = (da_ref[r, :] + db_ref[r, :]) * g_ref[...] * (1.0 / tokens)
        up = up - jnp.mean(up, -1, keepdims=True)
        means = mean_ref[r, :]
        invs = inv_ref[r, :]
        for t0 in range(0, tokens, group):
            mus, ivs, ks = [], [], []
            for t in range(t0, t0 + group):
                mu, iv = means[:, t : t + 1], invs[:, t : t + 1]
                x = f_ref[t, r, :].astype(F32)
                q = jnp.zeros((sub, 128), F32)
                for k in range(width // 128):
                    c = slice(k * 128, (k + 1) * 128)
                    q = q + (x[:, c] - mu) * up[:, c]
                proj = jnp.sum(q, -1, keepdims=True) * (1.0 / width)
                mus.append(mu)
                ivs.append(iv)
                ks.append(proj * iv * iv * iv)
            for j in range(group):
                x = f_ref[t0 + j, r, :].astype(F32)
                o_ref[t0 + j, r, :] = (ivs[j] * up - (x - mus[j]) * ks[j]).astype(BF16)
        return carry

    lax.fori_loop(0, rows // sub, step, 0)


def _ln_backward(ft, dpool_a, dpool_b, gamma, means, invs, rows=32, sub=32, group=7):
    tokens, images, width = ft.shape
    row_block = pl.BlockSpec((rows, width), lambda i: (i, 0))
    stat_block = pl.BlockSpec((rows, 128), lambda i: (i, 0))
    return pl.pallas_call(
        functools.partial(_df_kernel, rows=rows, sub=sub, group=group),
        grid=(images // rows,),
        in_specs=[
            pl.BlockSpec((tokens, rows, width), lambda i: (0, i, 0)),
            row_block,
            row_block,
            pl.BlockSpec((1, width), lambda i: (0, 0)),
            stat_block,
            stat_block,
        ],
        out_specs=pl.BlockSpec((tokens, rows, width), lambda i: (0, i, 0)),
        out_shape=jax.ShapeDtypeStruct((tokens, images, width), BF16),
        compiler_params=pltpu.CompilerParams(vmem_limit_bytes=60 * MIB),
        cost_estimate=_cost(45e-6 * 996e12, tokens * images * width * 4),
        name="ln_backward",
    )(ft, dpool_a, dpool_b, gamma, means, invs)


def _logits_kernel(base_ref, p_ref, w_ref, b_ref, y_ref, l_ref, st_ref, m_acc, s_acc, t_acc, v_acc, p16, *, tile, row_block):
    i = pl.program_id(0)

    @pl.when(i == 0)
    def _():
        m_acc[...] = jnp.full(m_acc.shape, -jnp.inf, F32)
        for acc in (s_acc, t_acc, v_acc):
            acc[...] = jnp.zeros(acc.shape, F32)
        p16[...] = p_ref[...].astype(BF16)

    col = base_ref[0] + i * tile + lax.broadcasted_iota(jnp.int32, (1, tile), 1)
    valid = col < VALID
    groups = [slice(k * 128, (k + 1) * 128) for k in range(tile // 128)]
    for r0 in range(0, p16.shape[0], row_block):
        r = slice(r0, r0 + row_block)
        raw = jnp.dot(p16[r, :], w_ref[...], preferred_element_type=F32) + b_ref[...]
        logit = jnp.where(valid, raw, -1e30)
        l_ref[r, :] = logit
        target = jnp.where(col == y_ref[r, :], logit, 0.0)
        kept = jnp.where(valid, raw, 0.0)
        m0 = m_acc[r, :]
        m = m0
        for g in groups:
            m = jnp.maximum(m, logit[:, g])
        s = s_acc[r, :] * jnp.exp(m0 - m)
        t, v = t_acc[r, :], v_acc[r, :]
        for g in groups:
            s = s + jnp.exp(logit[:, g] - m)
            t = t + target[:, g]
            v = v + kept[:, g]
        m_acc[r, :] = m
        s_acc[r, :] = s
        t_acc[r, :] = t
        v_acc[r, :] = v

    @pl.when(i == pl.num_programs(0) - 1)
    def _():
        m = m_acc[...]
        top = jnp.max(m, -1, keepdims=True)
        norm = jnp.sum(s_acc[...] * jnp.exp(m - top), -1, keepdims=True)
        target = jnp.sum(t_acc[...], -1, keepdims=True)
        total = jnp.sum(v_acc[...], -1, keepdims=True)
        lane = lax.broadcasted_iota(jnp.int32, (1, 128), 1)
        st_ref[...] = jnp.where(lane == 0, top, jnp.where(lane == 1, norm, jnp.where(lane == 2, target, total)))


def _own_logits(base, p, w, b, y, tile=1024, row_block=256):
    images, width = p.shape
    cols = w.shape[1]
    return pl.pallas_call(
        functools.partial(_logits_kernel, tile=tile, row_block=row_block),
        grid_spec=pltpu.PrefetchScalarGridSpec(
            num_scalar_prefetch=1,
            grid=(cols // tile,),
            in_specs=[
                pl.BlockSpec((images, width), lambda i, s: (0, 0)),
                pl.BlockSpec((width, tile), lambda i, s: (0, i)),
                pl.BlockSpec((1, tile), lambda i, s: (0, i)),
                pl.BlockSpec((images, 1), lambda i, s: (0, 0)),
            ],
            out_specs=[pl.BlockSpec((images, tile), lambda i, s: (0, i)), pl.BlockSpec((images, 128), lambda i, s: (0, 0))],
            scratch_shapes=[pltpu.VMEM((images, 128), F32)] * 4 + [pltpu.VMEM((images, width), BF16)],
        ),
        out_shape=[jax.ShapeDtypeStruct((images, cols), F32), jax.ShapeDtypeStruct((images, 128), F32)],
        compiler_params=pltpu.CompilerParams(vmem_limit_bytes=56 * MIB),
        cost_estimate=_cost(2 * images * width * cols, width * cols * 2 + images * cols * 4),
        name="own_logits",
    )(base, p, w, b, y)


def _dlogit(logit, shift, col, y, total):
    flat = SMOOTH / VALID / total
    drop = jnp.where(col == y, flat + (1.0 - SMOOTH) / total, flat)
    return jnp.where(col < VALID, jnp.exp(logit - shift) - drop, 0.0)


def _dpool_kernel(base_ref, l_ref, w_ref, shift_ref, y_ref, o_ref, *, tile, total):
    i = pl.program_id(0)
    col = base_ref[0] + i * tile + lax.broadcasted_iota(jnp.int32, (1, tile), 1)
    d = _dlogit(l_ref[...], shift_ref[...], col, y_ref[...], total).astype(BF16)
    part = lax.dot_general(d, w_ref[...], (((1,), (1,)), ((), ())), preferred_element_type=F32)

    @pl.when(i == 0)
    def _():
        o_ref[...] = part

    @pl.when(i > 0)
    def _():
        o_ref[...] += part


def _own_dpool(base, logits, w, shift, y, total, tile=1024):
    images, cols = logits.shape
    width = w.shape[0]
    column = pl.BlockSpec((images, 1), lambda i, s: (0, 0))
    return pl.pallas_call(
        functools.partial(_dpool_kernel, tile=tile, total=total),
        grid_spec=pltpu.PrefetchScalarGridSpec(
            num_scalar_prefetch=1,
            grid=(cols // tile,),
            in_specs=[
                pl.BlockSpec((images, tile), lambda i, s: (0, i)),
                pl.BlockSpec((width, tile), lambda i, s: (0, i)),
                column,
                column,
            ],
            out_specs=pl.BlockSpec((images, width), lambda i, s: (0, 0)),
        ),
        out_shape=jax.ShapeDtypeStruct((images, width), F32),
        compiler_params=pltpu.CompilerParams(vmem_limit_bytes=56 * MIB),
        cost_estimate=_cost(2 * images * width * cols, width * cols * 2 + images * cols * 4),
        name="own_dpool",
    )(base, logits, w, shift, y)


def _dw_kernel(sc_ref, *refs, counts, tile, row_block, total, has_acc, to_full, aliased, own, off):
    refs = list(refs)
    take = lambda n: [refs.pop(0) for _ in range(n)]
    p_refs = take(len(counts))
    w_ref, b_ref, shift_ref, y_ref = take(4)
    acc_ref, acc_db_ref = take(2) if has_acc else (None, None)
    got_ref = None
    if aliased:
        _, = take(1)
        if aliased > 1:
            got_ref, = take(1)
    full_ref, = take(1) if to_full else (None,)
    o_ref, db_ref = take(2)
    p16, d16 = refs
    i = pl.program_id(0)

    @pl.when(i == 0)
    def _():
        r0 = 0
        for ref, n in zip(p_refs, counts):
            p16[r0 : r0 + n, :] = ref[...].astype(BF16)
            r0 += n

    def compute():
        col = sc_ref[0] + (off + i) * tile + lax.broadcasted_iota(jnp.int32, (1, tile), 1)
        db = jnp.zeros((1, tile), F32)
        for r0 in range(0, p16.shape[0], row_block):
            r = slice(r0, r0 + row_block)
            logit = jnp.dot(p16[r, :], w_ref[...], preferred_element_type=F32) + b_ref[...]
            d = _dlogit(logit, shift_ref[r, :], col, y_ref[r, :], total)
            db = db + jnp.sum(d, 0, keepdims=True)
            d16[r, :] = d.astype(BF16)
        out = lax.dot_general(p16[...], d16[...], (((0,), (0,)), ((), ())), preferred_element_type=F32)
        if has_acc:
            out = out + acc_ref[...]
            db = db + acc_db_ref[...]
        o_ref[...] = out
        if to_full:
            full_ref[...] = out
        db_ref[...] = db

    if got_ref is None:
        compute()
    else:
        pl.when(i < own)(compute)

        @pl.when(i >= own)
        def _():
            full_ref[...] = got_ref[...]


def _dw_phase(sc, pooled, w, b, shift, y, total, acc=None, own=None, off=0, full=None, got=None, got_off=0, to_full=False, tile=512, row_block=256):
    counts = [p.shape[0] for p in pooled]
    images = sum(counts)
    width, cols = w.shape
    own = own or cols // 2 // tile
    extra = got.shape[1] // tile if got is not None else 0
    mine = lambda i: jnp.minimum(i, own - 1)
    theirs = lambda i: jnp.maximum(i - own, 0)
    in_specs = [pl.BlockSpec(p.shape, lambda i, s: (0, 0)) for p in pooled]
    in_specs += [
        pl.BlockSpec((width, tile), lambda i, s: (0, s[1] + off + mine(i))),
        pl.BlockSpec((1, tile), lambda i, s: (0, s[1] + off + mine(i))),
        pl.BlockSpec((images, 1), lambda i, s: (0, 0)),
        pl.BlockSpec((images, 1), lambda i, s: (0, 0)),
    ]
    args = list(pooled) + [w, b, shift, y]
    if acc is not None:
        in_specs += [pl.BlockSpec((width, tile), lambda i, s: (0, off + mine(i))), pl.BlockSpec((1, tile), lambda i, s: (0, off + mine(i)))]
        args += list(acc)
    aliases = {}
    aliased = 0
    if full is not None:
        aliased = 1
        aliases = {len(args) + 1: 0}
        in_specs.append(pl.BlockSpec(memory_space=pl.ANY))
        args.append(full)
    if got is not None:
        aliased = 2
        in_specs.append(pl.BlockSpec((width, tile), lambda i, s: (0, theirs(i))))
        args.append(got)
    out_specs = [pl.BlockSpec((width, tile), lambda i, s: (0, mine(i))), pl.BlockSpec((1, tile), lambda i, s: (0, mine(i)))]
    out_shape = [jax.ShapeDtypeStruct((width, own * tile), F32), jax.ShapeDtypeStruct((1, own * tile), F32)]
    if to_full:
        place = lambda i, s: (0, jnp.where(i < own, s[1] + off + i, s[2] + got_off + i - own))
        out_specs.insert(0, pl.BlockSpec((width, tile), place))
        out_shape.insert(0, jax.ShapeDtypeStruct((width, cols), F32))
    return pl.pallas_call(
        functools.partial(
            _dw_kernel, counts=counts, tile=tile, row_block=row_block, total=total, has_acc=acc is not None, to_full=to_full, aliased=aliased, own=own, off=off
        ),
        grid_spec=pltpu.PrefetchScalarGridSpec(
            num_scalar_prefetch=1,
            grid=(own + extra,),
            in_specs=in_specs,
            out_specs=out_specs,
            scratch_shapes=[pltpu.VMEM((images, width), BF16), pltpu.VMEM((images, tile), BF16)],
        ),
        out_shape=out_shape,
        input_output_aliases=aliases,
        compiler_params=pltpu.CompilerParams(vmem_limit_bytes=63 * MIB),
        cost_estimate=_cost(4.6 * images * width * own * tile, width * own * tile * 10),
        name="dw_phase",
    )(sc, *args)


def _place_kernel(sc_ref, full_in, *refs, starts):
    parts, full_ref = refs[:-1], refs[-1]
    i = pl.program_id(0)
    for ref, start, stop in zip(parts, starts[:-1], starts[1:]):

        @pl.when((i >= start) & (i < stop))
        def _():
            full_ref[...] = ref[...]


def _place(sc, full, parts, off, tile=512):
    width, cols = full.shape
    starts = [0]
    for part in parts:
        starts.append(starts[-1] + part.shape[1] // tile)
    specs = [
        pl.BlockSpec((width, tile), lambda i, s, lo=lo, hi=hi: (0, jnp.clip(i - lo, 0, hi - lo - 1))) for lo, hi in zip(starts[:-1], starts[1:])
    ]
    return pl.pallas_call(
        functools.partial(_place_kernel, starts=starts),
        grid_spec=pltpu.PrefetchScalarGridSpec(
            num_scalar_prefetch=1,
            grid=(starts[-1],),
            in_specs=[pl.BlockSpec(memory_space=pl.ANY)] + specs,
            out_specs=pl.BlockSpec((width, tile), lambda i, s: (0, s[2] + off + i)),
        ),
        out_shape=jax.ShapeDtypeStruct((width, cols), F32),
        input_output_aliases={1: 0},
        compiler_params=pltpu.CompilerParams(vmem_limit_bytes=60 * MIB),
        cost_estimate=_cost(6e-6 * 996e12, width * starts[-1] * tile * 8),
        name="place",
    )(sc, full, *parts)


CHUNKS = (3, 3, 3, 2)
TILE = 512


def solution(mesh):
    dp_size, tp_size = mesh.shape["dp"], mesh.shape["tp"]

    def swap(x, bit):
        return lax.ppermute(x, "dp", [(i, i ^ bit) for i in range(dp_size)])

    def head(feats, ln_gamma, ln_beta, w, b, labels):
        images, _, width = feats.shape
        cols = w.shape[1]
        total = images * dp_size
        tp_i, dp_i = lax.axis_index("tp"), lax.axis_index("dp")
        core = dp_i % 2
        half_tiles = cols // 2 // TILE
        base = (tp_i * cols).astype(jnp.int32).reshape(1)
        sc = jnp.stack([tp_i * cols + core * (cols // 2), core * half_tiles, (1 - core) * half_tiles]).astype(jnp.int32)
        ft = jnp.transpose(feats, (1, 0, 2))
        gamma, beta, bias = ln_gamma.reshape(1, width), ln_beta.reshape(1, width), b.reshape(1, cols)
        y_col = labels.reshape(images, 1)

        p, xm, means, invs = _ln_forward(ft, gamma, beta)
        p_core, p_x, p_y = swap(p, 1), swap(p, 2), swap(p, 4)

        logits, st = _own_logits(base, p, w, bias, y_col)
        rows = jnp.concatenate([st[:, :4].T, labels.astype(F32)[None], jnp.zeros((3, images), F32)], 0)
        every = lax.all_gather(rows, ("tp", "dp"))
        every = every.reshape(tp_size, dp_size, 8, images)
        top = jnp.max(every[:, :, 0], 0)
        lse = top + jnp.log(jnp.sum(every[:, :, 1] * jnp.exp(every[:, :, 0] - top), 0))
        target = jnp.sum(every[:, :, 2], 0)
        valid_sum = jnp.sum(every[:, :, 3], 0)
        loss = jnp.sum(lse - (1.0 - SMOOTH) * target - (SMOOTH / VALID) * valid_sum) / total
        shift_all = lse + jnp.log(F32(total))
        y_all = every[0, :, 4].astype(jnp.int32)

        def pick(bits):
            idx = dp_i ^ jnp.array(bits, jnp.int32)
            return shift_all[idx].reshape(-1, 1), y_all[idx].reshape(-1, 1)

        shift_own, _ = pick([0])
        dpool_a = _own_dpool(base, logits, w, shift_own, y_col, total)
        dpool_b = lax.ppermute(dpool_a, "tp", [(i, tp_size - 1 - i) for i in range(tp_size)])

        acc = _dw_phase(sc, [p, p_core], w, bias, *pick([0, 1]), total)
        acc = _dw_phase(sc, [p_x, p_y], w, bias, *pick([2, 4]), total, acc=acc)
        half = images // 2
        p_d = [swap(p_x[:half], 4), swap(p_y[half:], 2)]
        p_rest = [swap(p_x, 1), swap(p_y, 1)] + p_d
        p_rest += [swap(p_d[0], 1), swap(p_d[1], 1)]
        shift_rest, y_rest = pick([3, 5, 6, 7])

        full, sent, dbs, off = None, [], [], 0
        offs = []
        for c, n in enumerate(CHUNKS):
            got = sent[c - 2] if c >= 2 else None
            full, part, db = _dw_phase(
                sc, p_rest, w, bias, shift_rest, y_rest, total, acc=acc, own=n, off=off, full=full, got=got, got_off=offs[c - 2] if c >= 2 else 0, to_full=True
            )
            sent.append(swap(part, 1))
            dbs.append(db)
            offs.append(off)
            off += n

        db_mine = jnp.concatenate(dbs, 1)
        db_other = swap(db_mine, 1)
        grad_b = jnp.where(core == 0, jnp.concatenate([db_mine, db_other], 1), jnp.concatenate([db_other, db_mine], 1)).reshape(cols)

        dpool = dpool_a + dpool_b
        sums = jnp.stack([jnp.sum(dpool * xm, 0), jnp.sum(dpool, 0)])
        for bit in (1, 2, 4):
            sums = sums + swap(sums, bit)

        dft = _ln_backward(ft, dpool_a, dpool_b, gamma, means, invs)
        full = _place(sc, full, sent[-2:], offs[-2])
        return loss, jnp.transpose(dft, (1, 0, 2)), full, grad_b, sums[0], sums[1]

    return jax.shard_map(
        head,
        mesh=mesh,
        in_specs=(P("dp", None, None), P(), P(), P(None, "tp"), P("tp"), P("dp")),
        out_specs=(P(), P("dp", None, None), P(None, "tp"), P("tp"), P(), P()),
        check_vma=False,
    )
```

```python
import functools

import jax
import jax.numpy as jnp
from jax import lax
from jax.experimental import pallas as pl
from jax.experimental.pallas import tpu as pltpu
from jax.sharding import PartitionSpec as P


VALID = 21841
LN_EPS = 1e-5
SMOOTH = 0.1
F32 = jnp.float32
BF16 = jnp.bfloat16
MIB = 2**20


def _cost(flops, nbytes):
    return pl.CostEstimate(flops=int(flops), bytes_accessed=int(nbytes), transcendentals=0)


def _ln_kernel(f_ref, g_ref, b_ref, p_ref, xm_ref, mean_ref, inv_ref, *, rows, sub, group):
    lane = lax.broadcasted_iota(jnp.int32, (sub, 128), 1)
    tokens, _, width = f_ref.shape
    ones = jnp.ones((width, 128), BF16)

    def step(s, carry):
        r = pl.ds(pl.multiple_of(s * sub, sub), sub)
        acc = jnp.zeros((sub, width), F32)
        means = jnp.zeros((sub, 128), F32)
        invs = jnp.zeros((sub, 128), F32)
        for t0 in range(0, tokens, group):
            xb = f_ref[t0 : t0 + group, r, :].reshape(group * sub, width)
            mu_all = jnp.dot(xb, ones, preferred_element_type=F32) * (1.0 / width)
            mus, ivs = [], []
            for j in range(group):
                mu = mu_all[j * sub : (j + 1) * sub, :]
                x = f_ref[t0 + j, r, :].astype(F32)
                q = jnp.zeros((sub, 128), F32)
                for k in range(width // 128):
                    d = x[:, k * 128 : (k + 1) * 128] - mu
                    q = q + d * d
                var = jnp.sum(q, -1, keepdims=True) * (1.0 / width)
                mus.append(mu)
                ivs.append(lax.rsqrt(var + LN_EPS))
            for j in range(group):
                x = f_ref[t0 + j, r, :].astype(F32)
                hats = [(x[:, k * 128 : (k + 1) * 128] - mus[j]) * ivs[j] for k in range(width // 128)]
                acc = acc + jnp.concatenate(hats, 1)
                hit = lane == t0 + j
                means = jnp.where(hit, mus[j], means)
                invs = jnp.where(hit, ivs[j], invs)
        xm = acc * (1.0 / tokens)
        xm_ref[r, :] = xm
        p_ref[r, :] = (xm * g_ref[...] + b_ref[...]).astype(BF16).astype(F32)
        mean_ref[r, :] = means
        inv_ref[r, :] = invs
        return carry

    lax.fori_loop(0, rows // sub, step, 0)


def _ln_forward(ft, gamma, beta, rows=32, sub=32, group=7):
    tokens, images, width = ft.shape
    return pl.pallas_call(
        functools.partial(_ln_kernel, rows=rows, sub=sub, group=group),
        grid=(images // rows,),
        in_specs=[
            pl.BlockSpec((tokens, rows, width), lambda i: (0, i, 0)),
            pl.BlockSpec((1, width), lambda i: (0, 0)),
            pl.BlockSpec((1, width), lambda i: (0, 0)),
        ],
        out_specs=[pl.BlockSpec((rows, width), lambda i: (i, 0))] * 2 + [pl.BlockSpec((rows, 128), lambda i: (i, 0))] * 2,
        out_shape=[jax.ShapeDtypeStruct((images, width), F32)] * 2 + [jax.ShapeDtypeStruct((images, 128), F32)] * 2,
        compiler_params=pltpu.CompilerParams(vmem_limit_bytes=60 * MIB),
        cost_estimate=_cost(36e-6 * 996e12, tokens * images * width * 2),
        name="ln_forward",
    )(ft, gamma, beta)


def _df_kernel(f_ref, da_ref, db_ref, g_ref, mean_ref, inv_ref, o_ref, mu_all, iv_all, *, rows, sub, group):
    tokens, _, width = f_ref.shape
    lanes = [slice(k * 128, (k + 1) * 128) for k in range(width // 128)]

    def step(s, carry):
        r = pl.ds(pl.multiple_of(s * sub, sub), sub)
        up = (da_ref[r, :] + db_ref[r, :]) * g_ref[...] * (1.0 / tokens)
        up = up - jnp.mean(up, -1, keepdims=True)
        means = mean_ref[r, :]
        invs = inv_ref[r, :]
        for t in range(tokens):
            mu_all[t] = jnp.broadcast_to(means[:, t : t + 1], (sub, 128))
            iv_all[t] = jnp.broadcast_to(invs[:, t : t + 1], (sub, 128))
        for t0 in range(0, tokens, group):
            scales = []
            for t in range(t0, t0 + group):
                x = f_ref[t, r, :].astype(F32)
                mu, iv = mu_all[t], iv_all[t]
                q = jnp.zeros((sub, 128), F32)
                for c in lanes:
                    q = q + (x[:, c] - mu) * up[:, c]
                proj = jnp.sum(q, -1, keepdims=True) * (1.0 / width)
                scales.append(proj * iv * iv * iv)
            for t in range(t0, t0 + group):
                x = f_ref[t, r, :].astype(F32)
                mu, iv, k = mu_all[t], iv_all[t], scales[t - t0]
                o_ref[t, r, :] = jnp.concatenate([iv * up[:, c] - (x[:, c] - mu) * k for c in lanes], 1).astype(BF16)
        return carry

    lax.fori_loop(0, rows // sub, step, 0)


def _ln_backward(ft, dpool_a, dpool_b, gamma, means, invs, rows=64, sub=32, group=7):
    tokens, images, width = ft.shape
    row_block = pl.BlockSpec((rows, width), lambda i: (i, 0))
    stat_block = pl.BlockSpec((rows, 128), lambda i: (i, 0))
    return pl.pallas_call(
        functools.partial(_df_kernel, rows=rows, sub=sub, group=group),
        grid=(images // rows,),
        in_specs=[
            pl.BlockSpec((tokens, rows, width), lambda i: (0, i, 0)),
            row_block,
            row_block,
            pl.BlockSpec((1, width), lambda i: (0, 0)),
            stat_block,
            stat_block,
        ],
        out_specs=pl.BlockSpec((tokens, rows, width), lambda i: (0, i, 0)),
        out_shape=jax.ShapeDtypeStruct((tokens, images, width), BF16),
        scratch_shapes=[pltpu.VMEM((tokens, sub, 128), F32)] * 2,
        compiler_params=pltpu.CompilerParams(vmem_limit_bytes=60 * MIB),
        cost_estimate=_cost(45e-6 * 996e12, tokens * images * width * 4),
        name="ln_backward",
    )(ft, dpool_a, dpool_b, gamma, means, invs)


def _masked(w, bias, col):
    valid = col < VALID
    return jnp.where(valid, w, jnp.zeros((), BF16)), jnp.where(valid, bias, -1e30)


def _dlogit(logit, shift, col, y, total):
    flat = jnp.where(col < VALID, SMOOTH / VALID / total, 0.0)
    drop = jnp.where(col == y, (SMOOTH / VALID + 1.0 - SMOOTH) / total, flat)
    return jnp.exp(logit - shift) - drop


def _rows_to_columns(rows):
    return jnp.concatenate([rows] * 16, 0).T


def _head_kernel(p_ref, w_ref, b_ref, y_ref, o_ref, sh_ref, l_all, m_acc, s_acc, t_acc, v_acc, p16, mine, other, send, every, shift, zs, zr, ds, dr, *, tile, steps, row_block, total, dp_size):
    i = pl.program_id(0)
    tp_i, dp_i = lax.axis_index("tp"), lax.axis_index("dp")
    images = p16.shape[0]
    t = lax.rem(i, steps)
    col = tp_i * (tile * steps) + t * tile + lax.broadcasted_iota(jnp.int32, (1, tile), 1)
    lane = lax.broadcasted_iota(jnp.int32, (1, 128), 1)
    barrier = pltpu.get_barrier_semaphore()
    mesh_id = pl.DeviceIdType.MESH
    across = pltpu.make_async_remote_copy(mine, other, zs, zr, device_id=(1 - tp_i, dp_i), device_id_type=mesh_id)
    casts = [
        pltpu.make_async_remote_copy(
            send, every.at[dp_i], ds.at[j], dr.at[j], device_id=(tp_i, lax.rem(dp_i + j + 1, dp_size)), device_id_type=mesh_id
        )
        for j in range(dp_size - 1)
    ]

    @pl.when(i == 0)
    def _():
        pl.semaphore_signal(barrier, inc=1, device_id=(1 - tp_i, dp_i), device_id_type=mesh_id)
        for j in range(dp_size - 1):
            pl.semaphore_signal(barrier, inc=1, device_id=(tp_i, lax.rem(dp_i + j + 1, dp_size)), device_id_type=mesh_id)
        m_acc[...] = jnp.full(m_acc.shape, -jnp.inf, F32)
        for acc in (s_acc, t_acc, v_acc):
            acc[...] = jnp.zeros(acc.shape, F32)
        p16[...] = p_ref[...].astype(BF16)

    @pl.when(i < steps)
    def _():
        w, bias = _masked(w_ref[...], b_ref[...], col)
        groups = [slice(k * 128, (k + 1) * 128) for k in range(tile // 128)]
        bsum = jnp.zeros((1, 128), F32)
        kept = jnp.where(col < VALID, b_ref[...], 0.0)
        for g in groups:
            bsum = bsum + kept[:, g]
        for r0 in range(0, images, row_block):
            r = slice(r0, r0 + row_block)
            raw = jnp.dot(p16[r, :], w, preferred_element_type=F32)
            logit = raw + bias
            l_all[t, r, :] = logit
            target = jnp.where(col == y_ref[r, :], logit, 0.0)
            m0 = m_acc[r, :]
            m = m0
            for g in groups:
                m = jnp.maximum(m, logit[:, g])
            s = s_acc[r, :] * jnp.exp(m0 - m)
            tt, v = t_acc[r, :], v_acc[r, :] + bsum
            for g in groups:
                s = s + jnp.exp(logit[:, g] - m)
                tt = tt + target[:, g]
                v = v + raw[:, g]
            m_acc[r, :] = m
            s_acc[r, :] = s
            t_acc[r, :] = tt
            v_acc[r, :] = v

    @pl.when(i == steps - 1)
    def _():
        m = m_acc[...]
        top = jnp.max(m, -1, keepdims=True)
        norm = jnp.sum(s_acc[...] * jnp.exp(m - top), -1, keepdims=True)
        target = jnp.sum(t_acc[...], -1, keepdims=True)
        valid_sum = jnp.sum(v_acc[...], -1, keepdims=True)
        stats = jnp.where(lane == 0, top, jnp.where(lane == 1, norm, jnp.where(lane == 2, target, valid_sum)))
        mine[...] = stats.T[:8, :]

    @pl.when(i == steps)
    def _():
        pl.semaphore_wait(barrier, dp_size)
        across.start()
        across.wait()
        a, b = mine[...], other[...]
        top = jnp.maximum(a[0:1], b[0:1])
        lse = top + jnp.log(a[1:2] * jnp.exp(a[0:1] - top) + b[1:2] * jnp.exp(b[0:1] - top))
        loss = lse - (1.0 - SMOOTH) * (a[2:3] + b[2:3]) - (SMOOTH / VALID) * (a[3:4] + b[3:4])
        row = lax.broadcasted_iota(jnp.int32, (8, images), 0)
        rows = jnp.where(row == 0, lse + jnp.log(F32(total)), jnp.where(row == 1, loss, 0.0))
        cols = _rows_to_columns(rows)
        shift[...] = cols
        out = jnp.where(lane == 2, y_ref[...].astype(F32), cols)
        send[...] = out.T[:8, :]

    @pl.when(i == steps + 1)
    def _():
        every[dp_i] = send[...]
        for c in casts:
            c.start()

    @pl.when(i >= steps)
    def _():
        for r0 in range(0, images, row_block):
            r = slice(r0, r0 + row_block)
            d = _dlogit(l_all[t, r, :], shift[r, 0:1], col, y_ref[r, :], total).astype(BF16)
            part = lax.dot_general(d, w_ref[...], (((1,), (1,)), ((), ())), preferred_element_type=F32)
            o_ref[r, :] = jnp.where(i == steps, part, o_ref[r, :] + part)

    @pl.when(i == 2 * steps - 1)
    def _():
        for c in casts:
            c.wait()
        sh_ref[...] = every[...]


def _own_head(p, w, b, y, dp_size, tile=1024, row_block=256):
    images, width = p.shape
    cols = w.shape[1]
    steps = cols // tile
    dma = pltpu.SemaphoreType.DMA
    small = pltpu.VMEM((8, images), F32)
    return pl.pallas_call(
        functools.partial(_head_kernel, tile=tile, steps=steps, row_block=row_block, total=images * dp_size, dp_size=dp_size),
        grid=(2 * steps,),
        in_specs=[
            pl.BlockSpec((images, width), lambda i: (0, 0)),
            pl.BlockSpec((width, tile), lambda i: (0, lax.rem(i, steps))),
            pl.BlockSpec((1, tile), lambda i: (0, lax.rem(i, steps))),
            pl.BlockSpec((images, 1), lambda i: (0, 0)),
        ],
        out_specs=[pl.BlockSpec((images, width), lambda i: (0, 0)), pl.BlockSpec((dp_size, 8, images), lambda i: (0, 0, 0))],
        out_shape=[jax.ShapeDtypeStruct((images, width), F32), jax.ShapeDtypeStruct((dp_size, 8, images), F32)],
        scratch_shapes=[pltpu.VMEM((steps, images, tile), F32)]
        + [pltpu.VMEM((images, 128), F32)] * 4
        + [pltpu.VMEM((images, width), BF16), small, small, small, pltpu.VMEM((dp_size, 8, images), F32), pltpu.VMEM((images, 128), F32)]
        + [dma, dma, dma((dp_size - 1,)), dma((dp_size - 1,))],
        compiler_params=pltpu.CompilerParams(vmem_limit_bytes=60 * MIB, collective_id=0, has_side_effects=True),
        cost_estimate=_cost(4 * images * width * cols, width * cols * 4),
        name="own_head",
    )(p, w, b, y)


def _dw_kernel(sc_ref, *refs, counts, sets, tile, row_block, total, has_acc, to_full, aliased, give_p, plan, off):
    refs = list(refs)
    take = lambda n: [refs.pop(0) for _ in range(n)]
    p_refs = take(len(counts))
    sh_refs = take(sets)
    w_ref, b_ref = take(2)
    acc_ref, acc_db_ref = take(2) if has_acc else (None, None)
    got_ref = None
    if aliased:
        take(1)
        if aliased > 1:
            (got_ref,) = take(1)
    (full_ref,) = take(1) if to_full else (None,)
    o_ref, db_ref = take(2)
    (give_ref,) = take(1) if give_p else (None,)
    p16, d16, stat = refs[-3:] if p_refs[0].dtype != BF16 else (p_refs[0], *refs[-2:])
    images = d16.shape[0]
    i = pl.program_id(0)

    @pl.when(i == 0)
    def _():
        if p16 is not p_refs[0]:
            r0 = 0
            for ref, n in zip(p_refs, counts):
                p16[r0 : r0 + n, :] = ref[...].astype(BF16)
                r0 += n
            if give_p:
                give_ref[...] = p16[...]
        n = images // sets
        for k, ref in enumerate(sh_refs):
            stat[k * n : (k + 1) * n, :] = _rows_to_columns(ref[0])

    def compute():
        col = sc_ref[0] + (off + plan.own(i)) * tile + lax.broadcasted_iota(jnp.int32, (1, tile), 1)
        w, bias = _masked(w_ref[...], b_ref[...], col)
        db = jnp.zeros((1, tile), F32)
        for r0 in range(0, images, row_block):
            r = slice(r0, r0 + row_block)
            logit = jnp.dot(p16[r, :], w, preferred_element_type=F32) + bias
            d = _dlogit(logit, stat[r, 0:1], col, stat[r, 2:3].astype(jnp.int32), total)
            db = db + jnp.sum(d, 0, keepdims=True)
            d16[r, :] = d.astype(BF16)
        out = lax.dot_general(p16[...], d16[...], (((0,), (0,)), ((), ())), preferred_element_type=F32)
        if has_acc:
            out = out + acc_ref[...]
            db = db + acc_db_ref[...]
        o_ref[...] = out
        if to_full:
            full_ref[...] = out
        db_ref[...] = db

    if got_ref is None:
        compute()
    else:
        pl.when(plan.is_own(i))(compute)

        @pl.when(jnp.logical_not(plan.is_own(i)))
        def _():
            full_ref[...] = got_ref[...]


class _Plan:
    def __init__(self, own, extra):
        self.n, self.e, self.m = own, extra, min(own, extra)

    def is_own(self, i):
        tail = i >= 2 * self.m
        return jnp.where(tail, self.n > self.e, lax.rem(i, 2) == 0)

    def own(self, i):
        return jnp.minimum(jnp.where(i < 2 * self.m, (i + 1) // 2, i - self.m), self.n - 1)

    def last(self, i):
        return jnp.minimum(jnp.where(i < 2 * self.m, i // 2, i - self.m), self.n - 1)

    def copy(self, i):
        return jnp.clip(jnp.where(i < 2 * self.m, i // 2, i - self.m), 0, max(self.e - 1, 0))


def _dw_phase(sc, pooled, slots, shifts, w, b, total, acc=None, own=None, off=0, full=None, got=None, got_off=0, to_full=False, give_p=False, tile=512, row_block=512):
    counts = [p.shape[0] for p in pooled]
    images = sum(counts)
    width, cols = w.shape
    own = own or cols // 2 // tile
    plan = _Plan(own, got.shape[1] // tile if got is not None else 0)
    in_specs = [pl.BlockSpec(p.shape, lambda i, s: (0, 0)) for p in pooled]
    in_specs += [pl.BlockSpec((1, *shifts.shape[1:]), lambda i, s, k=k: (s[3 + k], 0, 0)) for k in slots]
    in_specs += [
        pl.BlockSpec((width, tile), lambda i, s: (0, s[1] + off + plan.own(i))),
        pl.BlockSpec((1, tile), lambda i, s: (0, s[1] + off + plan.own(i))),
    ]
    args = list(pooled) + [shifts] * len(slots) + [w, b]
    if acc is not None:
        in_specs += [pl.BlockSpec((width, tile), lambda i, s: (0, off + plan.own(i))), pl.BlockSpec((1, tile), lambda i, s: (0, off + plan.own(i)))]
        args += list(acc)
    aliases = {}
    aliased = 0
    if full is not None:
        aliased = 1
        aliases = {len(args) + 1: 0}
        in_specs.append(pl.BlockSpec(memory_space=pl.ANY))
        args.append(full)
    if got is not None:
        aliased = 2
        in_specs.append(pl.BlockSpec((width, tile), lambda i, s: (0, plan.copy(i))))
        args.append(got)
    out_specs = [pl.BlockSpec((width, tile), lambda i, s: (0, plan.last(i))), pl.BlockSpec((1, tile), lambda i, s: (0, plan.last(i)))]
    out_shape = [jax.ShapeDtypeStruct((width, own * tile), F32), jax.ShapeDtypeStruct((1, own * tile), F32)]
    if to_full:
        place = lambda i, s: (0, jnp.where(plan.is_own(i), s[1] + off + plan.last(i), s[2] + got_off + plan.copy(i)))
        out_specs.insert(0, pl.BlockSpec((width, tile), place))
        out_shape.insert(0, jax.ShapeDtypeStruct((width, cols), F32))
    if give_p:
        out_specs.append(pl.BlockSpec((images, width), lambda i, s: (0, 0)))
        out_shape.append(jax.ShapeDtypeStruct((images, width), BF16))
    scratch = [pltpu.VMEM((images, tile), BF16), pltpu.VMEM((images, 128), F32)]
    if pooled[0].dtype != BF16:
        scratch.insert(0, pltpu.VMEM((images, width), BF16))
    return pl.pallas_call(
        functools.partial(
            _dw_kernel,
            counts=counts,
            sets=len(slots),
            tile=tile,
            row_block=row_block,
            total=total,
            has_acc=acc is not None,
            to_full=to_full,
            aliased=aliased,
            give_p=give_p,
            plan=plan,
            off=off,
        ),
        grid_spec=pltpu.PrefetchScalarGridSpec(
            num_scalar_prefetch=1, grid=(plan.n + plan.e,), in_specs=in_specs, out_specs=out_specs, scratch_shapes=scratch
        ),
        out_shape=out_shape,
        input_output_aliases=aliases,
        compiler_params=pltpu.CompilerParams(vmem_limit_bytes=63 * MIB),
        cost_estimate=_cost(4.6 * images * width * own * tile, width * own * tile * 10),
        name="dw_phase",
    )(sc, *args)


def _place_kernel(sc_ref, full_in, *refs, starts):
    parts, full_ref = refs[:-1], refs[-1]
    i = pl.program_id(0)
    for ref, start, stop in zip(parts, starts[:-1], starts[1:]):

        @pl.when((i >= start) & (i < stop))
        def _():
            full_ref[...] = ref[...]


def _place(sc, full, parts, off, tile=512):
    width, cols = full.shape
    starts = [0]
    for part in parts:
        starts.append(starts[-1] + part.shape[1] // tile)
    specs = [
        pl.BlockSpec((width, tile), lambda i, s, lo=lo, hi=hi: (0, jnp.clip(i - lo, 0, hi - lo - 1))) for lo, hi in zip(starts[:-1], starts[1:])
    ]
    return pl.pallas_call(
        functools.partial(_place_kernel, starts=starts),
        grid_spec=pltpu.PrefetchScalarGridSpec(
            num_scalar_prefetch=1,
            grid=(starts[-1],),
            in_specs=[pl.BlockSpec(memory_space=pl.ANY)] + specs,
            out_specs=pl.BlockSpec((width, tile), lambda i, s: (0, s[2] + off + i)),
        ),
        out_shape=jax.ShapeDtypeStruct((width, cols), F32),
        input_output_aliases={1: 0},
        compiler_params=pltpu.CompilerParams(vmem_limit_bytes=60 * MIB),
        cost_estimate=_cost(6e-6 * 996e12, width * starts[-1] * tile * 8),
        name="place",
    )(sc, full, *parts)


CHUNKS = (3, 3, 3, 2)
TILE = 512


def solution(mesh):
    dp_size, tp_size = mesh.shape["dp"], mesh.shape["tp"]

    def swap(x, bit):
        return lax.ppermute(x, "dp", [(i, i ^ bit) for i in range(dp_size)])

    def head(feats, ln_gamma, ln_beta, w, b, labels):
        images, _, width = feats.shape
        cols = w.shape[1]
        total = images * dp_size
        tp_i, dp_i = lax.axis_index("tp"), lax.axis_index("dp")
        core = dp_i % 2
        half_tiles = cols // 2 // TILE
        bits = (0, 1, 2, 4, 3, 5, 6, 7)
        sc = jnp.stack([tp_i * cols + core * (cols // 2), core * half_tiles, (1 - core) * half_tiles] + [dp_i ^ k for k in bits]).astype(jnp.int32)
        ft = jnp.transpose(feats, (1, 0, 2))
        gamma, beta, bias = ln_gamma.reshape(1, width), ln_beta.reshape(1, width), b.reshape(1, cols)

        p, xm, means, invs = _ln_forward(ft, gamma, beta)
        p_core, p_x, p_y = swap(p, 1), swap(p, 2), swap(p, 4)

        dpool_a, shifts = _own_head(p, w, bias, labels.reshape(images, 1), dp_size)
        dpool_b = lax.ppermute(dpool_a, "tp", [(i, tp_size - 1 - i) for i in range(tp_size)])

        acc = _dw_phase(sc, [p, p_core], (0, 1), shifts, w, bias, total)
        acc = _dw_phase(sc, [p_x, p_y], (2, 3), shifts, w, bias, total, acc=acc)
        half = images // 2
        p_d = [swap(p_x[:half], 4), swap(p_y[half:], 2)]
        p_rest = [swap(p_x, 1), swap(p_y, 1)] + p_d
        p_rest += [swap(p_d[0], 1), swap(p_d[1], 1)]

        full, sent, dbs, offs, off = None, [], [], [], 0
        for c, n in enumerate(CHUNKS):
            got = sent[c - 2] if c >= 2 else None
            full, part, db, *rest = _dw_phase(
                sc,
                p_rest,
                (4, 5, 6, 7),
                shifts,
                w,
                bias,
                total,
                acc=acc,
                own=n,
                off=off,
                full=full,
                got=got,
                got_off=offs[c - 2] if c >= 2 else 0,
                to_full=True,
                give_p=c == 0,
            )
            p_rest = rest or p_rest
            sent.append(swap(part, 1))
            dbs.append(db)
            offs.append(off)
            off += n

        db_mine = jnp.concatenate(dbs, 1)
        db_other = swap(db_mine, 1)
        grad_b = jnp.where(core == 0, jnp.concatenate([db_mine, db_other], 1), jnp.concatenate([db_other, db_mine], 1)).reshape(cols)

        dpool = dpool_a + dpool_b
        loss_own = jnp.sum(lax.dynamic_index_in_dim(shifts, dp_i, 0, keepdims=False)[1])
        sums = jnp.stack([jnp.sum(dpool * xm, 0), jnp.sum(dpool, 0), jnp.broadcast_to(loss_own / total, (width,))])
        for bit in (1, 2, 4):
            sums = sums + swap(sums, bit)

        dft = _ln_backward(ft, dpool_a, dpool_b, gamma, means, invs)
        full = _place(sc, full, sent[-2:], offs[-2])
        return sums[2, 0], jnp.transpose(dft, (1, 0, 2)), full, grad_b, sums[0], sums[1]

    return jax.shard_map(
        head,
        mesh=mesh,
        in_specs=(P("dp", None, None), P(), P(), P(None, "tp"), P("tp"), P("dp")),
        out_specs=(P(), P("dp", None, None), P(None, "tp"), P("tp"), P(), P()),
        check_vma=False,
    )
```

```python
import functools

import jax
import jax.numpy as jnp
from jax import lax
from jax.experimental import pallas as pl
from jax.experimental.pallas import tpu as pltpu
from jax.sharding import PartitionSpec as P


VALID = 21841
LN_EPS = 1e-5
SMOOTH = 0.1
F32 = jnp.float32
BF16 = jnp.bfloat16
MIB = 2**20


def _cost(flops, nbytes):
    return pl.CostEstimate(flops=int(flops), bytes_accessed=int(nbytes), transcendentals=0)


def _ln_kernel(f_ref, g_ref, b_ref, p_ref, xm_ref, mean_ref, inv_ref, *, rows, sub):
    lane = lax.broadcasted_iota(jnp.int32, (sub, 128), 1)
    tokens, _, width = f_ref.shape

    def step(s, carry):
        r = pl.ds(pl.multiple_of(s * sub, sub), sub)
        acc = jnp.zeros((sub, width), F32)
        means = jnp.zeros((sub, 128), F32)
        invs = jnp.zeros((sub, 128), F32)
        for t in range(tokens):
            x = f_ref[t, r, :].astype(F32)
            mu = jnp.sum(x, -1, keepdims=True) * (1.0 / width)
            xc = x - mu
            iv = lax.rsqrt(jnp.sum(xc * xc, -1, keepdims=True) * (1.0 / width) + LN_EPS)
            acc = acc + xc * iv
            means = jnp.where(lane == t, mu, means)
            invs = jnp.where(lane == t, iv, invs)
        xm = acc * (1.0 / tokens)
        xm_ref[r, :] = xm
        p_ref[r, :] = (xm * g_ref[...] + b_ref[...]).astype(BF16).astype(F32)
        mean_ref[r, :] = means
        inv_ref[r, :] = invs
        return carry

    lax.fori_loop(0, rows // sub, step, 0)


def _ln_forward(ft, gamma, beta, rows=64, sub=16):
    tokens, images, width = ft.shape
    return pl.pallas_call(
        functools.partial(_ln_kernel, rows=rows, sub=sub),
        grid=(images // rows,),
        in_specs=[
            pl.BlockSpec((tokens, rows, width), lambda i: (0, i, 0)),
            pl.BlockSpec((1, width), lambda i: (0, 0)),
            pl.BlockSpec((1, width), lambda i: (0, 0)),
        ],
        out_specs=[pl.BlockSpec((rows, width), lambda i: (i, 0))] * 2 + [pl.BlockSpec((rows, 128), lambda i: (i, 0))] * 2,
        out_shape=[jax.ShapeDtypeStruct((images, width), F32)] * 2 + [jax.ShapeDtypeStruct((images, 128), F32)] * 2,
        compiler_params=pltpu.CompilerParams(vmem_limit_bytes=60 * MIB),
        cost_estimate=_cost(36e-6 * 996e12, tokens * images * width * 2),
        name="ln_forward",
    )(ft, gamma, beta)


def _df_rows(f_ref, da_ref, db_ref, g_ref, mean_ref, inv_ref, o_ref, mu_all, iv_all, r, group=7):
    tokens, _, width = f_ref.shape
    lanes = [slice(k * 128, (k + 1) * 128) for k in range(width // 128)]
    up = (da_ref[r, :] + db_ref[r, :]) * g_ref[...] * (1.0 / tokens)
    up = up - jnp.mean(up, -1, keepdims=True)
    means = mean_ref[r, :]
    invs = inv_ref[r, :]
    spread = (up.shape[0], 128)
    for t in range(tokens):
        mu_all[t, r, :] = jnp.broadcast_to(means[:, t : t + 1], spread)
        iv_all[t, r, :] = jnp.broadcast_to(invs[:, t : t + 1], spread)
    for t0 in range(0, tokens, group):
        scales = []
        for t in range(t0, t0 + group):
            x = f_ref[t, r, :].astype(F32)
            mu, iv = mu_all[t, r, :], iv_all[t, r, :]
            q = jnp.zeros(spread, F32)
            for c in lanes:
                q = q + (x[:, c] - mu) * up[:, c]
            proj = jnp.sum(q, -1, keepdims=True) * (1.0 / width)
            scales.append(proj * iv * iv * iv)
        for t in range(t0, t0 + group):
            x = f_ref[t, r, :].astype(F32)
            mu, iv, k = mu_all[t, r, :], iv_all[t, r, :], scales[t - t0]
            o_ref[t, r, :] = jnp.concatenate([iv * up[:, c] - (x[:, c] - mu) * k for c in lanes], 1).astype(BF16)


def _masked(w, bias, col):
    valid = col < VALID
    return jnp.where(valid, w, jnp.zeros((), BF16)), jnp.where(valid, bias, -1e30)


def _dlogit(logit, shift, col, y, total):
    flat = jnp.where(col < VALID, SMOOTH / VALID / total, 0.0)
    drop = jnp.where(col == y, (SMOOTH / VALID + 1.0 - SMOOTH) / total, flat)
    return jnp.exp(logit - shift) - drop


def _rows_to_columns(rows):
    return jnp.concatenate([rows] * 16, 0).T


def _head_kernel(p_ref, w_ref, b_ref, y_ref, o_ref, sh_ref, loss_ref, l_all, m_acc, s_acc, t_acc, v_acc, p16, mine, other, send, every, shift, zs, zr, ds, dr, *, tile, steps, row_block, total, dp_size):
    i = pl.program_id(0)
    tp_i, dp_i = lax.axis_index("tp"), lax.axis_index("dp")
    images = p16.shape[0]
    t = lax.rem(i, steps)
    col = tp_i * (tile * steps) + t * tile + lax.broadcasted_iota(jnp.int32, (1, tile), 1)
    lane = lax.broadcasted_iota(jnp.int32, (1, 128), 1)
    barrier = pltpu.get_barrier_semaphore()
    mesh_id = pl.DeviceIdType.MESH
    across = pltpu.make_async_remote_copy(mine, other, zs, zr, device_id=(1 - tp_i, dp_i), device_id_type=mesh_id)
    casts = [
        pltpu.make_async_remote_copy(
            send, every.at[dp_i], ds.at[j], dr.at[j], device_id=(tp_i, lax.rem(dp_i + j + 1, dp_size)), device_id_type=mesh_id
        )
        for j in range(dp_size - 1)
    ]

    @pl.when(i == 0)
    def _():
        pl.semaphore_signal(barrier, inc=1, device_id=(1 - tp_i, dp_i), device_id_type=mesh_id)
        for j in range(dp_size - 1):
            pl.semaphore_signal(barrier, inc=1, device_id=(tp_i, lax.rem(dp_i + j + 1, dp_size)), device_id_type=mesh_id)
        m_acc[...] = jnp.full(m_acc.shape, -jnp.inf, F32)
        for acc in (s_acc, t_acc, v_acc):
            acc[...] = jnp.zeros(acc.shape, F32)
        p16[...] = p_ref[...].astype(BF16)

    @pl.when(i < steps)
    def _():
        w, bias = _masked(w_ref[...], b_ref[...], col)
        groups = [slice(k * 128, (k + 1) * 128) for k in range(tile // 128)]
        bsum = jnp.zeros((1, 128), F32)
        kept = jnp.where(col < VALID, b_ref[...], 0.0)
        for g in groups:
            bsum = bsum + kept[:, g]
        for r0 in range(0, images, row_block):
            r = slice(r0, r0 + row_block)
            raw = jnp.dot(p16[r, :], w, preferred_element_type=F32)
            logit = raw + bias
            l_all[t, r, :] = logit
            target = jnp.where(col == y_ref[r, :], logit, 0.0)
            m0 = m_acc[r, :]
            m = m0
            for g in groups:
                m = jnp.maximum(m, logit[:, g])
            s = s_acc[r, :] * jnp.exp(m0 - m)
            tt, v = t_acc[r, :], v_acc[r, :] + bsum
            for g in groups:
                s = s + jnp.exp(logit[:, g] - m)
                tt = tt + target[:, g]
                v = v + raw[:, g]
            m_acc[r, :] = m
            s_acc[r, :] = s
            t_acc[r, :] = tt
            v_acc[r, :] = v

    @pl.when(i == steps - 1)
    def _():
        m = m_acc[...]
        top = jnp.max(m, -1, keepdims=True)
        norm = jnp.sum(s_acc[...] * jnp.exp(m - top), -1, keepdims=True)
        target = jnp.sum(t_acc[...], -1, keepdims=True)
        valid_sum = jnp.sum(v_acc[...], -1, keepdims=True)
        stats = jnp.where(lane == 0, top, jnp.where(lane == 1, norm, jnp.where(lane == 2, target, valid_sum)))
        mine[...] = stats.T[:8, :]

    @pl.when(i == steps)
    def _():
        pl.semaphore_wait(barrier, dp_size)
        across.start()
        across.wait()
        a, b = mine[...], other[...]
        top = jnp.maximum(a[0:1], b[0:1])
        lse = top + jnp.log(a[1:2] * jnp.exp(a[0:1] - top) + b[1:2] * jnp.exp(b[0:1] - top))
        loss = lse - (1.0 - SMOOTH) * (a[2:3] + b[2:3]) - (SMOOTH / VALID) * (a[3:4] + b[3:4])
        row = lax.broadcasted_iota(jnp.int32, (8, images), 0)
        rows = jnp.where(row == 0, lse + jnp.log(F32(total)), jnp.where(row == 1, loss, 0.0))
        cols = _rows_to_columns(rows)
        shift[...] = cols
        loss_ref[...] = loss
        out = jnp.where(lane == 2, y_ref[...].astype(F32), cols)
        send[...] = out.T[:8, :]

    @pl.when(i == steps + 1)
    def _():
        every[dp_i] = send[...]
        for c in casts:
            c.start()

    @pl.when(i >= steps)
    def _():
        for r0 in range(0, images, row_block):
            r = slice(r0, r0 + row_block)
            d = _dlogit(l_all[t, r, :], shift[r, 0:1], col, y_ref[r, :], total).astype(BF16)
            part = lax.dot_general(d, w_ref[...], (((1,), (1,)), ((), ())), preferred_element_type=F32)
            o_ref[r, :] = jnp.where(i == steps, part, o_ref[r, :] + part)

    @pl.when(i == 2 * steps - 1)
    def _():
        for c in casts:
            c.wait()
        sh_ref[...] = every[...]


def _own_head(p, w, b, y, dp_size, tile=2816, row_block=256):
    images, width = p.shape
    cols = w.shape[1]
    steps = cols // tile
    dma = pltpu.SemaphoreType.DMA
    small = pltpu.VMEM((8, images), F32)
    return pl.pallas_call(
        functools.partial(_head_kernel, tile=tile, steps=steps, row_block=row_block, total=images * dp_size, dp_size=dp_size),
        grid=(2 * steps,),
        in_specs=[
            pl.BlockSpec((images, width), lambda i: (0, 0)),
            pl.BlockSpec((width, tile), lambda i: (0, lax.rem(i, steps))),
            pl.BlockSpec((1, tile), lambda i: (0, lax.rem(i, steps))),
            pl.BlockSpec((images, 1), lambda i: (0, 0)),
        ],
        out_specs=[pl.BlockSpec((images, width), lambda i: (0, 0)), pl.BlockSpec((dp_size, 8, images), lambda i: (0, 0, 0)), pl.BlockSpec((1, images), lambda i: (0, 0))],
        out_shape=[jax.ShapeDtypeStruct((images, width), F32), jax.ShapeDtypeStruct((dp_size, 8, images), F32), jax.ShapeDtypeStruct((1, images), F32)],
        scratch_shapes=[pltpu.VMEM((steps, images, tile), F32)]
        + [pltpu.VMEM((images, 128), F32)] * 4
        + [pltpu.VMEM((images, width), BF16), small, small, small, pltpu.VMEM((dp_size, 8, images), F32), pltpu.VMEM((images, 128), F32)]
        + [dma, dma, dma((dp_size - 1,)), dma((dp_size - 1,))],
        compiler_params=pltpu.CompilerParams(vmem_limit_bytes=60 * MIB, collective_id=0, has_side_effects=True),
        cost_estimate=_cost(4 * images * width * cols, width * cols * 4),
        name="own_head",
    )(p, w, b, y)


DF_ROWS = 48
DF_SUB = 16


def _dw_kernel(sc_ref, *refs, counts, sets, tile, row_block, total, has_acc, aliased, to_full, give_p, off):
    refs = list(refs)
    take = lambda n: [refs.pop(0) for _ in range(n)]
    p_refs = take(len(counts))
    sh_refs = take(sets)
    w_ref, b_ref = take(2)
    acc_ref, acc_db_ref = take(2) if has_acc else (None, None)
    ln_refs = take(6) if to_full else None
    take(2 if aliased else 0)
    full_ref, df_ref = take(2) if to_full else (None, None)
    o_ref, db_ref = take(2)
    (give_ref,) = take(1) if give_p else (None,)
    d16, stat = take(2)
    mu_all, iv_all = take(2) if to_full else (None, None)
    p16 = refs[0] if refs else p_refs[0]
    images = d16.shape[0]
    i = pl.program_id(0)

    @pl.when(i == 0)
    def _():
        if p16 is not p_refs[0]:
            r0 = 0
            for ref, n in zip(p_refs, counts):
                p16[r0 : r0 + n, :] = ref[...].astype(BF16)
                r0 += n
            if give_p:
                give_ref[...] = p16[...]
        n = images // sets
        for k, ref in enumerate(sh_refs):
            stat[k * n : (k + 1) * n, :] = _rows_to_columns(ref[0])

    col = sc_ref[0] + (off + i) * tile + lax.broadcasted_iota(jnp.int32, (1, tile), 1)
    w, bias = _masked(w_ref[...], b_ref[...], col)
    db = jnp.zeros((1, tile), F32)
    for r0 in range(0, images, row_block):
        r = slice(r0, r0 + row_block)
        logit = jnp.dot(p16[r, :], w, preferred_element_type=F32) + bias
        d = _dlogit(logit, stat[r, 0:1], col, stat[r, 2:3].astype(jnp.int32), total)
        db = db + jnp.sum(d, 0, keepdims=True)
        d16[r, :] = d.astype(BF16)
    if to_full:
        for r0 in range(0, DF_ROWS, DF_SUB):
            _df_rows(*ln_refs, df_ref, mu_all, iv_all, slice(r0, r0 + DF_SUB))
    out = lax.dot_general(p16[...], d16[...], (((0,), (0,)), ((), ())), preferred_element_type=F32)
    if has_acc:
        out = out + acc_ref[...]
        db = db + acc_db_ref[...]
    o_ref[...] = out
    if to_full:
        full_ref[...] = out
    db_ref[...] = db


def _dw_phase(sc, pooled, slots, shifts, w, b, total, acc=None, own=None, off=0, ln=None, so_far=None, give_p=False, tile=512, row_block=512):
    counts = [p.shape[0] for p in pooled]
    images = sum(counts)
    width, cols = w.shape
    own = own or cols // 2 // tile
    const = lambda shape: pl.BlockSpec(shape, lambda i, s: (0, 0))
    in_specs = [const(p.shape) for p in pooled]
    in_specs += [pl.BlockSpec((1, *shifts.shape[1:]), lambda i, s, k=k: (s[3 + k], 0, 0)) for k in slots]
    in_specs += [pl.BlockSpec((width, tile), lambda i, s: (0, s[1] + off + i)), pl.BlockSpec((1, tile), lambda i, s: (0, s[1] + off + i))]
    args = list(pooled) + [shifts] * len(slots) + [w, b]
    if acc is not None:
        in_specs += [pl.BlockSpec((width, tile), lambda i, s: (0, off + i)), pl.BlockSpec((1, tile), lambda i, s: (0, off + i))]
        args += list(acc)
    out_specs = [pl.BlockSpec((width, tile), lambda i, s: (0, i)), pl.BlockSpec((1, tile), lambda i, s: (0, i))]
    out_shape = [jax.ShapeDtypeStruct((width, own * tile), F32), jax.ShapeDtypeStruct((1, own * tile), F32)]
    scratch = [pltpu.VMEM((images, tile), BF16), pltpu.VMEM((images, 128), F32)]
    aliases = {}
    flops, nbytes = 4.6 * images * width * own * tile, width * own * tile * 10
    if ln is not None:
        tokens = ln[0].shape[0]
        f_block = pl.BlockSpec((tokens, DF_ROWS, width), lambda i, s: (0, off + i, 0))
        rows = pl.BlockSpec((DF_ROWS, width), lambda i, s: (off + i, 0))
        stats = pl.BlockSpec((DF_ROWS, 128), lambda i, s: (off + i, 0))
        in_specs += [f_block, rows, rows, const((1, width)), stats, stats]
        args += list(ln)
        if so_far is not None:
            aliases = {len(args) + 1: 0, len(args) + 2: 1}
            in_specs += [pl.BlockSpec(memory_space=pl.ANY)] * 2
            args += list(so_far)
        out_specs = [pl.BlockSpec((width, tile), lambda i, s: (0, s[1] + off + i)), f_block] + out_specs
        out_shape = [jax.ShapeDtypeStruct((width, cols), F32), jax.ShapeDtypeStruct(ln[0].shape, BF16)] + out_shape
        scratch += [pltpu.VMEM((tokens, DF_ROWS, 128), F32)] * 2
        nbytes += own * DF_ROWS * tokens * width * 4
    if give_p:
        out_specs.append(const((images, width)))
        out_shape.append(jax.ShapeDtypeStruct((images, width), BF16))
    if pooled[0].dtype != BF16:
        scratch.append(pltpu.VMEM((images, width), BF16))
    return pl.pallas_call(
        functools.partial(
            _dw_kernel,
            counts=counts,
            sets=len(slots),
            tile=tile,
            row_block=row_block,
            total=total,
            has_acc=acc is not None,
            aliased=so_far is not None,
            to_full=ln is not None,
            give_p=give_p,
            off=off,
        ),
        grid_spec=pltpu.PrefetchScalarGridSpec(num_scalar_prefetch=1, grid=(own,), in_specs=in_specs, out_specs=out_specs, scratch_shapes=scratch),
        out_shape=out_shape,
        input_output_aliases=aliases,
        compiler_params=pltpu.CompilerParams(vmem_limit_bytes=67043328),
        cost_estimate=_cost(flops, nbytes),
        name="dw_phase",
    )(sc, *args)


def _place_kernel(sc_ref, full_in, *refs, pieces, slots, tile):
    *parts, full_ref, buf, in_sem, out_sem = refs
    height = buf.shape[1]
    ins, outs = [], []
    for k, (part, row, src, dst) in enumerate(pieces):
        slot = k % slots
        rows = pl.ds(row * height, height)
        col = pl.multiple_of((sc_ref[2] + dst) * tile, tile)
        ins.append(pltpu.make_async_copy(parts[part].at[rows, pl.ds(src * tile, tile)], buf.at[slot], in_sem.at[slot]))
        outs.append(pltpu.make_async_copy(buf.at[slot], full_ref.at[rows, pl.ds(col, tile)], out_sem.at[slot]))
    n, half = len(pieces), slots // 2
    for k in range(min(half, n)):
        ins[k].start()
    for k in range(n):
        ins[k].wait()
        outs[k].start()
        ahead = k + half
        if ahead < n:
            if ahead >= slots:
                outs[ahead - slots].wait()
            ins[ahead].start()
    for k in range(max(0, n - slots), n):
        outs[k].wait()


def _place(sc, full, parts, off, tile=512, split=4, slots=24):
    width = full.shape[0]
    pieces, dst = [], off
    for k, part in enumerate(parts):
        for src in range(part.shape[1] // tile):
            pieces += [(k, row, src, dst) for row in range(split)]
            dst += 1
    anywhere = pl.BlockSpec(memory_space=pl.ANY)
    return pl.pallas_call(
        functools.partial(_place_kernel, pieces=pieces, slots=slots, tile=tile),
        grid_spec=pltpu.PrefetchScalarGridSpec(
            num_scalar_prefetch=1,
            grid=(1,),
            in_specs=[anywhere] * (1 + len(parts)),
            out_specs=anywhere,
            scratch_shapes=[pltpu.VMEM((slots, width // split, tile), F32), pltpu.SemaphoreType.DMA((slots,)), pltpu.SemaphoreType.DMA((slots,))],
        ),
        out_shape=jax.ShapeDtypeStruct(full.shape, F32),
        input_output_aliases={1: 0},
        compiler_params=pltpu.CompilerParams(vmem_limit_bytes=60 * MIB),
        cost_estimate=_cost(6e-6 * 996e12, 8 * tile * width * (dst - off)),
        name="place",
    )(sc, full, *parts)


CHUNKS = (8, 3)
TILE = 512


def solution(mesh):
    dp_size, tp_size = mesh.shape["dp"], mesh.shape["tp"]

    def swap(x, bit):
        return lax.ppermute(x, "dp", [(i, i ^ bit) for i in range(dp_size)])

    def head(feats, ln_gamma, ln_beta, w, b, labels):
        images, _, width = feats.shape
        cols = w.shape[1]
        total = images * dp_size
        tp_i, dp_i = lax.axis_index("tp"), lax.axis_index("dp")
        core = dp_i % 2
        half_tiles = cols // 2 // TILE
        bits = (0, 1, 2, 4, 3, 5, 6, 7)
        sc = jnp.stack([tp_i * cols + core * (cols // 2), core * half_tiles, (1 - core) * half_tiles] + [dp_i ^ k for k in bits]).astype(jnp.int32)
        ft = jnp.transpose(feats, (1, 0, 2))
        gamma, beta, bias = ln_gamma.reshape(1, width), ln_beta.reshape(1, width), b.reshape(1, cols)

        p, xm, means, invs = _ln_forward(ft, gamma, beta)
        p_x, p_y, p_core = swap(p, 2), swap(p, 4), swap(p, 1)

        dpool_a, shifts, loss_rows = _own_head(p, w, bias, labels.reshape(images, 1), dp_size)
        p_d = swap(lax.optimization_barrier((p, loss_rows))[0], 6)
        dpool_b = lax.ppermute(dpool_a, "tp", [(i, tp_size - 1 - i) for i in range(tp_size)])

        acc = _dw_phase(sc, [p, p_core, p_x, p_y], (0, 1, 2, 3), shifts, w, bias, total)
        p_rest = [swap(p_x, 1), swap(p_y, 1), p_d, swap(p_d, 1)]

        so_far, sent, dbs, off = None, [], [], 0
        ln = (ft, dpool_a, dpool_b, gamma, means, invs)
        for c, n in enumerate(CHUNKS):
            full, dft, part, db, *rest = _dw_phase(
                sc, p_rest, (4, 5, 6, 7), shifts, w, bias, total, acc=acc, own=n, off=off, ln=ln, so_far=so_far, give_p=c == 0
            )
            so_far = (full, dft)
            p_rest = rest or p_rest
            sent.append(swap(part, 1))
            dbs.append(db)
            off += n

        db_mine = jnp.concatenate(dbs, 1)
        db_other = swap(db_mine, 1)
        grad_b = jnp.where(core == 0, jnp.concatenate([db_mine, db_other], 1), jnp.concatenate([db_other, db_mine], 1)).reshape(cols)

        dpool = dpool_a + dpool_b
        loss_own = jnp.sum(loss_rows)
        sums = jnp.stack([jnp.sum(dpool * xm, 0), jnp.sum(dpool, 0), jnp.broadcast_to(loss_own / total, (width,))])
        for bit in (1, 2, 4):
            sums = sums + swap(sums, bit)

        full = _place(sc, full, sent[:-1], 0)
        full = _place(sc, full, sent[-1:], off - CHUNKS[-1])
        return sums[2, 0], jnp.transpose(dft, (1, 0, 2)), full, grad_b, sums[0], sums[1]

    return jax.shard_map(
        head,
        mesh=mesh,
        in_specs=(P("dp", None, None), P(), P(), P(None, "tp"), P("tp"), P("dp")),
        out_specs=(P(), P("dp", None, None), P(None, "tp"), P("tp"), P(), P()),
        check_vma=False,
    )
```

```python
import functools

import jax
import jax.numpy as jnp
from jax import lax
from jax.experimental import pallas as pl
from jax.experimental.pallas import tpu as pltpu
from jax.sharding import PartitionSpec as P


VALID = 21841
LN_EPS = 1e-5
SMOOTH = 0.1
F32 = jnp.float32
BF16 = jnp.bfloat16
MIB = 2**20


def _cost(flops, nbytes):
    return pl.CostEstimate(flops=int(flops), bytes_accessed=int(nbytes), transcendentals=0)


def _ln_kernel(f_ref, g_ref, b_ref, p_ref, xm_ref, mean_ref, inv_ref, *, rows, sub):
    lane = lax.broadcasted_iota(jnp.int32, (sub, 128), 1)
    tokens, _, width = f_ref.shape

    def step(s, carry):
        r = pl.ds(pl.multiple_of(s * sub, sub), sub)
        acc = jnp.zeros((sub, width), F32)
        means = jnp.zeros((sub, 128), F32)
        invs = jnp.zeros((sub, 128), F32)
        for t in range(tokens):
            x = f_ref[t, r, :].astype(F32)
            mu = jnp.sum(x, -1, keepdims=True) * (1.0 / width)
            xc = x - mu
            iv = lax.rsqrt(jnp.sum(xc * xc, -1, keepdims=True) * (1.0 / width) + LN_EPS)
            acc = acc + xc * iv
            means = jnp.where(lane == t, mu, means)
            invs = jnp.where(lane == t, iv, invs)
        xm = acc * (1.0 / tokens)
        xm_ref[r, :] = xm
        p_ref[r, :] = (xm * g_ref[...] + b_ref[...]).astype(BF16).astype(F32)
        mean_ref[r, :] = means
        inv_ref[r, :] = invs
        return carry

    lax.fori_loop(0, rows // sub, step, 0)


def _ln_forward(ft, gamma, beta, rows=32, sub=16):
    tokens, images, width = ft.shape
    return pl.pallas_call(
        functools.partial(_ln_kernel, rows=rows, sub=sub),
        grid=(images // rows,),
        in_specs=[
            pl.BlockSpec((tokens, rows, width), lambda i: (0, i, 0)),
            pl.BlockSpec((1, width), lambda i: (0, 0)),
            pl.BlockSpec((1, width), lambda i: (0, 0)),
        ],
        out_specs=[pl.BlockSpec((rows, width), lambda i: (i, 0))] * 2 + [pl.BlockSpec((rows, 128), lambda i: (i, 0))] * 2,
        out_shape=[jax.ShapeDtypeStruct((images, width), F32)] * 2 + [jax.ShapeDtypeStruct((images, 128), F32)] * 2,
        compiler_params=pltpu.CompilerParams(vmem_limit_bytes=60 * MIB),
        cost_estimate=_cost(36e-6 * 996e12, tokens * images * width * 2),
        name="ln_forward",
    )(ft, gamma, beta)


def _df_rows(f_ref, da_ref, db_ref, g_ref, mean_ref, inv_ref, o_ref, mu_all, iv_all, r, group=7):
    tokens, _, width = f_ref.shape
    lanes = [slice(k * 128, (k + 1) * 128) for k in range(width // 128)]
    up = (da_ref[r, :] + db_ref[r, :]) * g_ref[...] * (1.0 / tokens)
    up = up - jnp.mean(up, -1, keepdims=True)
    means = mean_ref[r, :]
    invs = inv_ref[r, :]
    up_sum = jnp.sum(up, -1, keepdims=True)
    spread = (up.shape[0], 128)
    for t in range(tokens):
        mu_all[t, r, :] = jnp.broadcast_to(means[:, t : t + 1], spread)
        iv_all[t, r, :] = jnp.broadcast_to(invs[:, t : t + 1], spread)
    for t0 in range(0, tokens, group):
        scales = []
        for t in range(t0, t0 + group):
            x = f_ref[t, r, :].astype(F32)
            mu, iv = mu_all[t, r, :], iv_all[t, r, :]
            q = jnp.zeros(spread, F32)
            for c in lanes:
                q = q + x[:, c] * up[:, c]
            proj = (jnp.sum(q, -1, keepdims=True) - mu * up_sum) * (1.0 / width)
            scales.append(proj * iv * iv * iv)
        for t in range(t0, t0 + group):
            x = f_ref[t, r, :].astype(F32)
            mu, iv, k = mu_all[t, r, :], iv_all[t, r, :], scales[t - t0]
            o_ref[t, r, :] = jnp.concatenate([iv * up[:, c] - (x[:, c] - mu) * k for c in lanes], 1).astype(BF16)


def _masked(w, bias, col):
    valid = col < VALID
    return jnp.where(valid, w, jnp.zeros((), BF16)), jnp.where(valid, bias, -1e30)


def _dlogit(logit, shift, col, y, total):
    flat = jnp.where(col < VALID, SMOOTH / VALID / total, 0.0)
    drop = jnp.where(col == y, (SMOOTH / VALID + 1.0 - SMOOTH) / total, flat)
    return jnp.exp(logit - shift) - drop


def _rows_to_columns(rows):
    return jnp.concatenate([rows] * 16, 0).T


def _head_kernel(p_ref, w_ref, b_ref, y_ref, o_ref, sh_ref, loss_ref, l_all, m_acc, s_acc, t_acc, v_acc, p16, mine, other, send, every, shift, zs, zr, ds, dr, *, tile, steps, row_block, total, dp_size):
    i = pl.program_id(0)
    tp_i, dp_i = lax.axis_index("tp"), lax.axis_index("dp")
    images = p16.shape[0]
    t = lax.rem(i, steps)
    col = tp_i * (tile * steps) + t * tile + lax.broadcasted_iota(jnp.int32, (1, tile), 1)
    lane = lax.broadcasted_iota(jnp.int32, (1, 128), 1)
    barrier = pltpu.get_barrier_semaphore()
    mesh_id = pl.DeviceIdType.MESH
    across = pltpu.make_async_remote_copy(mine, other, zs, zr, device_id=(1 - tp_i, dp_i), device_id_type=mesh_id)
    casts = [
        pltpu.make_async_remote_copy(
            send, every.at[dp_i], ds.at[j], dr.at[j], device_id=(tp_i, lax.rem(dp_i + j + 1, dp_size)), device_id_type=mesh_id
        )
        for j in range(dp_size - 1)
    ]

    @pl.when(i == 0)
    def _():
        pl.semaphore_signal(barrier, inc=1, device_id=(1 - tp_i, dp_i), device_id_type=mesh_id)
        for j in range(dp_size - 1):
            pl.semaphore_signal(barrier, inc=1, device_id=(tp_i, lax.rem(dp_i + j + 1, dp_size)), device_id_type=mesh_id)
        m_acc[...] = jnp.full(m_acc.shape, -jnp.inf, F32)
        for acc in (s_acc, t_acc, v_acc):
            acc[...] = jnp.zeros(acc.shape, F32)
        p16[...] = p_ref[...].astype(BF16)

    @pl.when(i < steps)
    def _():
        w, bias = _masked(w_ref[...], b_ref[...], col)
        groups = [slice(k * 128, (k + 1) * 128) for k in range(tile // 128)]
        bsum = jnp.zeros((1, 128), F32)
        kept = jnp.where(col < VALID, b_ref[...], 0.0)
        for g in groups:
            bsum = bsum + kept[:, g]
        for r0 in range(0, images, row_block):
            r = slice(r0, r0 + row_block)
            raw = jnp.dot(p16[r, :], w, preferred_element_type=F32)
            logit = raw + bias
            l_all[t, r, :] = logit
            target = jnp.where(col == y_ref[r, :], logit, 0.0)
            m0 = m_acc[r, :]
            m = m0
            for g in groups:
                m = jnp.maximum(m, logit[:, g])
            s = s_acc[r, :] * jnp.exp(m0 - m)
            tt, v = t_acc[r, :], v_acc[r, :] + bsum
            for g in groups:
                s = s + jnp.exp(logit[:, g] - m)
                tt = tt + target[:, g]
                v = v + raw[:, g]
            m_acc[r, :] = m
            s_acc[r, :] = s
            t_acc[r, :] = tt
            v_acc[r, :] = v

    @pl.when(i == steps - 1)
    def _():
        m = m_acc[...]
        top = jnp.max(m, -1, keepdims=True)
        norm = jnp.sum(s_acc[...] * jnp.exp(m - top), -1, keepdims=True)
        target = jnp.sum(t_acc[...], -1, keepdims=True)
        valid_sum = jnp.sum(v_acc[...], -1, keepdims=True)
        stats = jnp.where(lane == 0, top, jnp.where(lane == 1, norm, jnp.where(lane == 2, target, valid_sum)))
        mine[...] = stats.T[:8, :]

    @pl.when(i == steps)
    def _():
        pl.semaphore_wait(barrier, dp_size)
        across.start()
        across.wait()
        a, b = mine[...], other[...]
        top = jnp.maximum(a[0:1], b[0:1])
        lse = top + jnp.log(a[1:2] * jnp.exp(a[0:1] - top) + b[1:2] * jnp.exp(b[0:1] - top))
        loss = lse - (1.0 - SMOOTH) * (a[2:3] + b[2:3]) - (SMOOTH / VALID) * (a[3:4] + b[3:4])
        row = lax.broadcasted_iota(jnp.int32, (8, images), 0)
        rows = jnp.where(row == 0, lse + jnp.log(F32(total)), jnp.where(row == 1, loss, 0.0))
        cols = _rows_to_columns(rows)
        shift[...] = cols
        loss_ref[...] = loss
        out = jnp.where(lane == 2, y_ref[...].astype(F32), cols)
        send[...] = out.T[:8, :]

    @pl.when(i == steps + 1)
    def _():
        every[dp_i] = send[...]
        for c in casts:
            c.start()

    @pl.when(i >= steps)
    def _():
        for r0 in range(0, images, row_block):
            r = slice(r0, r0 + row_block)
            d = _dlogit(l_all[t, r, :], shift[r, 0:1], col, y_ref[r, :], total).astype(BF16)
            part = lax.dot_general(d, w_ref[...], (((1,), (1,)), ((), ())), preferred_element_type=F32)
            o_ref[r, :] = jnp.where(i == steps, part, o_ref[r, :] + part)

    @pl.when(i == 2 * steps - 1)
    def _():
        for c in casts:
            c.wait()
        sh_ref[...] = every[...]


def _own_head(p, w, b, y, dp_size, tile=2816, row_block=256):
    images, width = p.shape
    cols = w.shape[1]
    steps = cols // tile
    dma = pltpu.SemaphoreType.DMA
    small = pltpu.VMEM((8, images), F32)
    return pl.pallas_call(
        functools.partial(_head_kernel, tile=tile, steps=steps, row_block=row_block, total=images * dp_size, dp_size=dp_size),
        grid=(2 * steps,),
        in_specs=[
            pl.BlockSpec((images, width), lambda i: (0, 0)),
            pl.BlockSpec((width, tile), lambda i: (0, lax.rem(i, steps))),
            pl.BlockSpec((1, tile), lambda i: (0, lax.rem(i, steps))),
            pl.BlockSpec((images, 1), lambda i: (0, 0)),
        ],
        out_specs=[pl.BlockSpec((images, width), lambda i: (0, 0)), pl.BlockSpec((dp_size, 8, images), lambda i: (0, 0, 0)), pl.BlockSpec((1, images), lambda i: (0, 0))],
        out_shape=[jax.ShapeDtypeStruct((images, width), F32), jax.ShapeDtypeStruct((dp_size, 8, images), F32), jax.ShapeDtypeStruct((1, images), F32)],
        scratch_shapes=[pltpu.VMEM((steps, images, tile), F32)]
        + [pltpu.VMEM((images, 128), F32)] * 4
        + [pltpu.VMEM((images, width), BF16), small, small, small, pltpu.VMEM((dp_size, 8, images), F32), pltpu.VMEM((images, 128), F32)]
        + [dma, dma, dma((dp_size - 1,)), dma((dp_size - 1,))],
        compiler_params=pltpu.CompilerParams(vmem_limit_bytes=60 * MIB, collective_id=0, has_side_effects=True),
        cost_estimate=_cost(4 * images * width * cols, width * cols * 4),
        name="own_head",
    )(p, w, b, y)


DF_ROWS = 48
DF_SUB = 16


def _dw_kernel(sc_ref, *refs, counts, sets, tile, row_block, total, has_acc, aliased, to_full, give_p, off):
    refs = list(refs)
    take = lambda n: [refs.pop(0) for _ in range(n)]
    p_refs = take(len(counts))
    sh_refs = take(sets)
    w_ref, b_ref = take(2)
    acc_ref, acc_db_ref = take(2) if has_acc else (None, None)
    ln_refs = take(6) if to_full else None
    take(2 if aliased else 0)
    full_ref, df_ref = take(2) if to_full else (None, None)
    o_ref, db_ref = take(2)
    (give_ref,) = take(1) if give_p else (None,)
    d16, shift_all, y_all = take(3)
    mu_all, iv_all = take(2) if to_full else (None, None)
    p16 = refs[0] if refs else p_refs[0]
    images = d16.shape[0]
    i = pl.program_id(0)

    @pl.when(i == 0)
    def _():
        if p16 is not p_refs[0]:
            r0 = 0
            for ref, n in zip(p_refs, counts):
                p16[r0 : r0 + n, :] = ref[...].astype(BF16)
                r0 += n
            if give_p:
                give_ref[...] = p16[...]
        n = images // sets
        for k, ref in enumerate(sh_refs):
            r, cols = slice(k * n, (k + 1) * n), _rows_to_columns(ref[0])
            shift_all[r, :] = jnp.broadcast_to(cols[:, 0:1], (n, 128))
            y_all[r, :] = jnp.broadcast_to(cols[:, 2:3], (n, 128)).astype(jnp.int32)

    col = sc_ref[0] + (off + i) * tile + lax.broadcasted_iota(jnp.int32, (1, tile), 1)
    w, bias = _masked(w_ref[...], b_ref[...], col)
    db = jnp.zeros((1, tile), F32)
    for r0 in range(0, images, row_block):
        r = slice(r0, r0 + row_block)
        logit = jnp.dot(p16[r, :], w, preferred_element_type=F32) + bias
        wide = lambda a: jnp.concatenate([a] * (tile // 128), 1)
        d = _dlogit(logit, wide(shift_all[r, :]), col, wide(y_all[r, :]), total)
        db = db + jnp.sum(d, 0, keepdims=True)
        d16[r, :] = d.astype(BF16)
    if to_full:
        for r0 in range(0, DF_ROWS, DF_SUB):
            _df_rows(*ln_refs, df_ref, mu_all, iv_all, slice(r0, r0 + DF_SUB))
    out = lax.dot_general(p16[...], d16[...], (((0,), (0,)), ((), ())), preferred_element_type=F32)
    if has_acc:
        out = out + acc_ref[...]
        db = db + acc_db_ref[...]
    o_ref[...] = out
    if to_full:
        full_ref[...] = out
    db_ref[...] = db


def _dw_phase(sc, pooled, slots, shifts, w, b, total, acc=None, own=None, off=0, ln=None, so_far=None, give_p=False, tile=512, row_block=512):
    counts = [p.shape[0] for p in pooled]
    images = sum(counts)
    width, cols = w.shape
    own = own or cols // 2 // tile
    const = lambda shape: pl.BlockSpec(shape, lambda i, s: (0, 0))
    in_specs = [const(p.shape) for p in pooled]
    in_specs += [pl.BlockSpec((1, *shifts.shape[1:]), lambda i, s, k=k: (s[3 + k], 0, 0)) for k in slots]
    in_specs += [pl.BlockSpec((width, tile), lambda i, s: (0, s[1] + off + i)), pl.BlockSpec((1, tile), lambda i, s: (0, s[1] + off + i))]
    args = list(pooled) + [shifts] * len(slots) + [w, b]
    if acc is not None:
        in_specs += [pl.BlockSpec((width, tile), lambda i, s: (0, off + i)), pl.BlockSpec((1, tile), lambda i, s: (0, off + i))]
        args += list(acc)
    out_specs = [pl.BlockSpec((width, tile), lambda i, s: (0, i)), pl.BlockSpec((1, tile), lambda i, s: (0, i))]
    out_shape = [jax.ShapeDtypeStruct((width, own * tile), F32), jax.ShapeDtypeStruct((1, own * tile), F32)]
    scratch = [pltpu.VMEM((images, tile), BF16), pltpu.VMEM((images, 128), F32), pltpu.VMEM((images, 128), jnp.int32)]
    aliases = {}
    flops, nbytes = 4.6 * images * width * own * tile, width * own * tile * 10
    if ln is not None:
        tokens = ln[0].shape[0]
        f_block = pl.BlockSpec((tokens, DF_ROWS, width), lambda i, s: (0, off + i, 0))
        rows = pl.BlockSpec((DF_ROWS, width), lambda i, s: (off + i, 0))
        stats = pl.BlockSpec((DF_ROWS, 128), lambda i, s: (off + i, 0))
        in_specs += [f_block, rows, rows, const((1, width)), stats, stats]
        args += list(ln)
        if so_far is not None:
            aliases = {len(args) + 1: 0, len(args) + 2: 1}
            in_specs += [pl.BlockSpec(memory_space=pl.ANY)] * 2
            args += list(so_far)
        out_specs = [pl.BlockSpec((width, tile), lambda i, s: (0, s[1] + off + i)), f_block] + out_specs
        out_shape = [jax.ShapeDtypeStruct((width, cols), F32), jax.ShapeDtypeStruct(ln[0].shape, BF16)] + out_shape
        scratch += [pltpu.VMEM((tokens, DF_ROWS, 128), F32)] * 2
        nbytes += own * DF_ROWS * tokens * width * 4
    if give_p:
        out_specs.append(const((images, width)))
        out_shape.append(jax.ShapeDtypeStruct((images, width), BF16))
    if pooled[0].dtype != BF16:
        scratch.append(pltpu.VMEM((images, width), BF16))
    return pl.pallas_call(
        functools.partial(
            _dw_kernel,
            counts=counts,
            sets=len(slots),
            tile=tile,
            row_block=row_block,
            total=total,
            has_acc=acc is not None,
            aliased=so_far is not None,
            to_full=ln is not None,
            give_p=give_p,
            off=off,
        ),
        grid_spec=pltpu.PrefetchScalarGridSpec(num_scalar_prefetch=1, grid=(own,), in_specs=in_specs, out_specs=out_specs, scratch_shapes=scratch),
        out_shape=out_shape,
        input_output_aliases=aliases,
        compiler_params=pltpu.CompilerParams(vmem_limit_bytes=67043328),
        cost_estimate=_cost(flops, nbytes),
        name="dw_phase",
    )(sc, *args)


def _place_kernel(sc_ref, full_in, *refs, pieces, slots, tile):
    *parts, full_ref, buf, in_sem, out_sem = refs
    height = buf.shape[1]
    ins, outs = [], []
    for k, (part, row, src, dst) in enumerate(pieces):
        slot = k % slots
        rows = pl.ds(row * height, height)
        col = pl.multiple_of((sc_ref[2] + dst) * tile, tile)
        ins.append(pltpu.make_async_copy(parts[part].at[rows, pl.ds(src * tile, tile)], buf.at[slot], in_sem.at[slot]))
        outs.append(pltpu.make_async_copy(buf.at[slot], full_ref.at[rows, pl.ds(col, tile)], out_sem.at[slot]))
    n, half = len(pieces), slots // 2
    for k in range(min(half, n)):
        ins[k].start()
    for k in range(n):
        ins[k].wait()
        outs[k].start()
        ahead = k + half
        if ahead < n:
            if ahead >= slots:
                outs[ahead - slots].wait()
            ins[ahead].start()
    for k in range(max(0, n - slots), n):
        outs[k].wait()


def _place(sc, full, parts, off, tile=512, split=4, slots=24):
    width = full.shape[0]
    pieces, dst = [], off
    for k, part in enumerate(parts):
        for src in range(part.shape[1] // tile):
            pieces += [(k, row, src, dst) for row in range(split)]
            dst += 1
    anywhere = pl.BlockSpec(memory_space=pl.ANY)
    return pl.pallas_call(
        functools.partial(_place_kernel, pieces=pieces, slots=slots, tile=tile),
        grid_spec=pltpu.PrefetchScalarGridSpec(
            num_scalar_prefetch=1,
            grid=(1,),
            in_specs=[anywhere] * (1 + len(parts)),
            out_specs=anywhere,
            scratch_shapes=[pltpu.VMEM((slots, width // split, tile), F32), pltpu.SemaphoreType.DMA((slots,)), pltpu.SemaphoreType.DMA((slots,))],
        ),
        out_shape=jax.ShapeDtypeStruct(full.shape, F32),
        input_output_aliases={1: 0},
        compiler_params=pltpu.CompilerParams(vmem_limit_bytes=60 * MIB),
        cost_estimate=_cost(6e-6 * 996e12, 8 * tile * width * (dst - off)),
        name="place",
    )(sc, full, *parts)


CHUNKS = (8, 3)
TILE = 512


def solution(mesh):
    dp_size, tp_size = mesh.shape["dp"], mesh.shape["tp"]

    def swap(x, bit):
        return lax.ppermute(x, "dp", [(i, i ^ bit) for i in range(dp_size)])

    def head(feats, ln_gamma, ln_beta, w, b, labels):
        images, _, width = feats.shape
        cols = w.shape[1]
        total = images * dp_size
        tp_i, dp_i = lax.axis_index("tp"), lax.axis_index("dp")
        core = dp_i % 2
        half_tiles = cols // 2 // TILE
        bits = (0, 1, 2, 4, 3, 5, 6, 7)
        sc = jnp.stack([tp_i * cols + core * (cols // 2), core * half_tiles, (1 - core) * half_tiles] + [dp_i ^ k for k in bits]).astype(jnp.int32)
        ft = jnp.transpose(feats, (1, 0, 2))
        gamma, beta, bias = ln_gamma.reshape(1, width), ln_beta.reshape(1, width), b.reshape(1, cols)

        p, xm, means, invs = _ln_forward(ft, gamma, beta)
        p_x, p_y, p_core = swap(p, 2), swap(p, 4), swap(p, 1)

        dpool_a, shifts, loss_rows = _own_head(p, w, bias, labels.reshape(images, 1), dp_size)
        p_d = swap(lax.optimization_barrier((p, loss_rows))[0], 6)
        dpool_b = lax.ppermute(dpool_a, "tp", [(i, tp_size - 1 - i) for i in range(tp_size)])

        acc = _dw_phase(sc, [p, p_core, p_x, p_y], (0, 1, 2, 3), shifts, w, bias, total)
        p_rest = [swap(p_x, 1), swap(p_y, 1), p_d, swap(p_d, 1)]

        so_far, sent, dbs, off = None, [], [], 0
        ln = (ft, dpool_a, dpool_b, gamma, means, invs)
        for c, n in enumerate(CHUNKS):
            full, dft, part, db, *rest = _dw_phase(
                sc, p_rest, (4, 5, 6, 7), shifts, w, bias, total, acc=acc, own=n, off=off, ln=ln, so_far=so_far, give_p=c == 0
            )
            so_far = (full, dft)
            p_rest = rest or p_rest
            sent.append(swap(part, 1))
            dbs.append(db)
            off += n

        db_mine = jnp.concatenate(dbs, 1)
        db_other = swap(db_mine, 1)
        grad_b = jnp.where(core == 0, jnp.concatenate([db_mine, db_other], 1), jnp.concatenate([db_other, db_mine], 1)).reshape(cols)

        dpool = dpool_a + dpool_b
        loss_own = jnp.sum(loss_rows)
        sums = jnp.stack([jnp.sum(dpool * xm, 0), jnp.sum(dpool, 0), jnp.broadcast_to(loss_own / total, (width,))])
        for bit in (1, 2, 4):
            sums = sums + swap(sums, bit)

        full = _place(sc, full, sent[:-1], 0)
        full = _place(sc, full, sent[-1:], off - CHUNKS[-1])
        return sums[2, 0], jnp.transpose(dft, (1, 0, 2)), full, grad_b, sums[0], sums[1]

    return jax.shard_map(
        head,
        mesh=mesh,
        in_specs=(P("dp", None, None), P(), P(), P(None, "tp"), P("tp"), P("dp")),
        out_specs=(P(), P("dp", None, None), P(None, "tp"), P("tp"), P(), P()),
        check_vma=False,
    )
```
